16 devices in a mesh: replica: 2 (over y, z), model: 8 (over x, core).
Axes of the slice: x: 4, y: 2, z: 1, core: 2. Of those that a mesh axis runs over, the one named last changes fastest.
The devices are a block of a 4x4x8 slice.
Arguments:
- x: bfloat16 [256, 16384], P('replica'), parts along dimension 0
- w_query: bfloat16 [16384, 16384], P(None, 'model')
- w_key: bfloat16 [16384, 1024], replicated
- w_value: bfloat16 [16384, 1024], replicated
- w_out: bfloat16 [16384, 16384], P('model')
- k_cache: bfloat16 [256, 8, 256, 128], P('replica'), parts along dimension 0
- v_cache: bfloat16 [256, 8, 256, 128], P('replica'), parts along dimension 0
- lengths: int32 [256], P('replica'), parts along dimension 0
Outputs:
- output 1: bfloat16 [256, 16384], P('replica'), parts along dimension 0
- output 2: bfloat16 [256, 8, 128], P('replica'), parts along dimension 0
- output 3: bfloat16 [256, 8, 128], P('replica'), parts along dimension 0
There are 2 independent parts. The reference program is written for one: setup_inputs(seed, part) draws one part's arguments, and reference() takes and returns one part's arrays. A program takes and returns all parts, laid end to end along the dimension named above; an argument that names none is the same for every part.
All inputs are finite; a program needn't handle non-finite values.
Results may differ from the reference program's by a relative error of at most 0.00333699.
Values are sent between devices in bfloat16 or wider.
A program may use at most 768 MiB of HBM per device.

```python
import jax
import jax.numpy as jnp
from jax import lax

D_MODEL = 16384
NUM_HEADS = 128
KV_HEADS = 8
HEAD_DIM = 128
BATCH_SIZE = 128
CONTEXT_LEN = 256


def draw_lengths(rng_key):
    key_perm, key_long, key_short = jax.random.split(rng_key, 3)
    perm_rank = jax.random.permutation(key_perm, BATCH_SIZE)
    long_count = max(1, BATCH_SIZE // 16)
    long_len = jax.random.randint(key_long, (BATCH_SIZE,), CONTEXT_LEN // 2, CONTEXT_LEN)
    short_len = jax.random.randint(key_short, (BATCH_SIZE,), 1, 33)
    seq_lens = jnp.where(perm_rank < 2 + long_count, long_len, short_len)
    seq_lens = jnp.where(perm_rank == 1, 1, seq_lens)
    seq_lens = jnp.where(perm_rank == 0, CONTEXT_LEN - 1, seq_lens)
    return seq_lens.astype(jnp.int32)


def setup_inputs(seed: int = 0, part: int = 0) -> dict:
    base_key = jax.random.key(seed)
    key_wq, key_wk, key_wv, key_wo = jax.random.split(base_key, 4)
    part_key = jax.random.fold_in(jax.random.key(seed + 1), part)
    key_x, key_kc, key_vc, key_mean, key_len = jax.random.split(part_key, 5)
    q_width = NUM_HEADS * HEAD_DIM
    kv_width = KV_HEADS * HEAD_DIM
    cache_shape = (BATCH_SIZE, KV_HEADS, CONTEXT_LEN, HEAD_DIM)
    x = jax.random.normal(key_x, (BATCH_SIZE, D_MODEL), jnp.float32).astype(jnp.bfloat16)
    w_query = (jax.random.normal(key_wq, (D_MODEL, q_width), jnp.float32) * D_MODEL ** -0.5).astype(jnp.bfloat16)
    w_key = (jax.random.normal(key_wk, (D_MODEL, kv_width), jnp.float32) * D_MODEL ** -0.5).astype(jnp.bfloat16)
    w_value = (jax.random.normal(key_wv, (D_MODEL, kv_width), jnp.float32) * D_MODEL ** -0.5).astype(jnp.bfloat16)
    w_out = (jax.random.normal(key_wo, (q_width, D_MODEL), jnp.float32) * q_width ** -0.5).astype(jnp.bfloat16)
    k_cache = (1.25 * jax.random.normal(key_kc, cache_shape, jnp.float32)).astype(jnp.bfloat16)
    v_mean = jax.random.normal(key_mean, (BATCH_SIZE, KV_HEADS, 1, HEAD_DIM), jnp.float32)
    v_cache = (jax.random.normal(key_vc, cache_shape, jnp.float32) + v_mean).astype(jnp.bfloat16)
    lengths = draw_lengths(key_len)
    return {"x": x, "w_query": w_query, "w_key": w_key, "w_value": w_value, "w_out": w_out, "k_cache": k_cache, "v_cache": v_cache, "lengths": lengths}


def reference(x, w_query, w_key, w_value, w_out, k_cache, v_cache, lengths):
    group_size = NUM_HEADS // KV_HEADS
    inv_sqrt = HEAD_DIM ** -0.5
    q_all = jnp.dot(x, w_query, preferred_element_type=jnp.float32).astype(jnp.bfloat16)
    k_new = jnp.dot(x, w_key, preferred_element_type=jnp.float32).astype(jnp.bfloat16).reshape(BATCH_SIZE, KV_HEADS, HEAD_DIM)
    v_new = jnp.dot(x, w_value, preferred_element_type=jnp.float32).astype(jnp.bfloat16).reshape(BATCH_SIZE, KV_HEADS, HEAD_DIM)
    q_heads = q_all.reshape(BATCH_SIZE, KV_HEADS, group_size, HEAD_DIM)
    positions = jnp.arange(CONTEXT_LEN)

    def one_sequence(item):
        q_seq, k_rows, v_rows, k_one, v_one, seq_len = item
        q_f32 = q_seq.astype(jnp.float32)
        scores = jnp.einsum("grd,gtd->grt", q_f32, k_rows.astype(jnp.float32)) * inv_sqrt
        score_new = jnp.einsum("grd,gd->gr", q_f32, k_one.astype(jnp.float32)) * inv_sqrt
        in_range = positions[None, None, :] < seq_len
        scores = jnp.where(in_range, scores, -jnp.inf)
        row_max = jnp.maximum(jnp.max(scores, axis=-1), score_new)
        weights = jnp.exp(scores - row_max[:, :, None])
        weight_new = jnp.exp(score_new - row_max)
        norm_sum = jnp.sum(weights, axis=-1) + weight_new
        out_sum = jnp.einsum("grt,gtd->grd", weights.astype(jnp.bfloat16).astype(jnp.float32), v_rows.astype(jnp.float32))
        out_sum = out_sum + weight_new.astype(jnp.bfloat16).astype(jnp.float32)[:, :, None] * v_one.astype(jnp.float32)[:, None, :]
        return (out_sum / norm_sum[:, :, None]).astype(jnp.bfloat16)

    attn_out = lax.map(one_sequence, (q_heads, k_cache, v_cache, k_new, v_new, lengths))
    o_flat = attn_out.reshape(BATCH_SIZE, NUM_HEADS * HEAD_DIM)
    y = (x.astype(jnp.float32) + jnp.dot(o_flat, w_out, preferred_element_type=jnp.float32)).astype(jnp.bfloat16)
    return (y, k_new, v_new)
```

```python
import functools

import jax
import jax.numpy as jnp
from jax import lax
from jax.experimental import pallas as pl
from jax.experimental.pallas import tpu as pltpu
from jax.sharding import PartitionSpec as P

MESH = pl.DeviceIdType.MESH
CORES = 2
ROUNDS = 8
OFFSETS = (2, 1, 3, 0)
BF16 = jnp.bfloat16
F32 = jnp.float32


def attend(queries, k_rows, v_rows, k_one, v_one, seq_lens):
    inv_sqrt = queries.shape[-1] ** -0.5
    scores = jnp.einsum("brd,btd->brt", queries, k_rows, preferred_element_type=F32) * inv_sqrt
    score_new = jnp.einsum("brd,bd->br", queries, k_one, preferred_element_type=F32) * inv_sqrt
    positions = jnp.arange(k_rows.shape[1])
    in_range = positions[None, None, :] < seq_lens[:, None, None]
    scores = jnp.where(in_range, scores, -jnp.inf)
    row_max = jnp.maximum(jnp.max(scores, axis=-1), score_new)
    weights = jnp.exp(scores - row_max[..., None])
    weight_new = jnp.exp(score_new - row_max)
    norm_sum = jnp.sum(weights, axis=-1) + weight_new
    out_sum = jnp.einsum("brt,btd->brd", weights.astype(BF16), v_rows, preferred_element_type=F32)
    out_sum = out_sum + weight_new.astype(BF16).astype(F32)[..., None] * v_one.astype(F32)[:, None, :]
    return (out_sum / norm_sum[..., None]).astype(BF16)


def out_kernel(size, o_ref, kv_ref, x_ref, w_ref, y_ref, kvs_ref,
               wbuf, xbuf, part, pair, hop, near,
               w_sem, x_sem, kv_sem, pair_send, pair_recv, hop_send, hop_recv, near_send, near_recv,
               ag_send, ag_recv, fwd_send, fwd_recv):
    me = lax.axis_index("model")
    core = lax.rem(me, CORES)
    chip = me // CORES
    chips = size // CORES
    plus = lax.rem(me + CORES, size)
    minus = lax.rem(me + size - CORES, size)
    mate = me + 1 - 2 * core
    plus2 = lax.rem(me + 2 * CORES, size)
    rows, depth = o_ref.shape
    half = rows // 2
    n, nk = part.shape[-1], kv_ref.shape[1]
    width = n * size
    top, bottom = pl.ds(0, half), pl.ds(half, half)
    kv_round = ROUNDS

    def slab(r, j):
        dest = lax.rem(chip + OFFSETS[j], chips)
        cols = pl.ds(pl.multiple_of(r * width + dest * (CORES * n), CORES * n), CORES * n)
        return pltpu.make_async_copy(w_ref.at[:, cols], wbuf.at[j], w_sem.at[j])

    def own_x(r):
        cols = pl.ds(pl.multiple_of(r * width + me * n, n), n)
        return pltpu.make_async_copy(x_ref.at[:, cols], xbuf.at[r], x_sem.at[r])

    def remote(src, dst, send, recv, to):
        return pltpu.make_async_remote_copy(
            src_ref=src, dst_ref=dst, send_sem=send, recv_sem=recv,
            device_id={"model": to}, device_id_type=MESH)

    def pair_copy(r, j):
        return remote(part.at[r, j, 1 - core], pair.at[r, j], pair_send.at[r, j], pair_recv.at[r, j], mate)

    def hop_copy(r, way):
        to, lines = ((plus, top), (minus, bottom))[way]
        return remote(part.at[r, 0, core, lines], hop.at[r, way], hop_send.at[r, way], hop_recv.at[r, way], to)

    def near_copy(r, way, late):
        to = (plus, minus)[way]
        lines = top if (way == 0) == late else bottom
        k = 2 * way + int(late)
        return remote(part.at[r, 1 + way, core, lines], near.at[r, way, lines],
                      near_send.at[r, k], near_recv.at[r, k], to)

    def block(r, owner, lines):
        if r is None:
            return kvs_ref.at[lines, pl.ds(pl.multiple_of(owner * nk, nk), nk)]
        return y_ref.at[lines, pl.ds(pl.multiple_of(r * width + owner * n, n), n)]

    everything = pl.ds(0, rows)

    def gather_copy(r, k):
        i = kv_round if r is None else r
        ref = block(r, me, everything)
        return remote(ref, ref, ag_send.at[i, k], ag_recv.at[i, k], (mate, plus, minus)[k])

    def relay_copy(r, way):
        i = kv_round if r is None else r
        ref = block(r, (minus, plus)[way], (top, bottom)[way])
        return remote(ref, ref, ag_send.at[i, 3 + way], ag_recv.at[i, 3 + way], (plus, minus)[way])

    def relayed_recv(r, way):
        i = kv_round if r is None else r
        ref = block(r, plus2, (top, bottom)[way])
        return remote(ref, ref, ag_send.at[i, 3 + way], ag_recv.at[i, 3 + way], (plus, minus)[way])

    def received(r, k):
        i = kv_round if r is None else r
        ref = block(r, (mate, minus, plus)[k], everything)
        return remote(ref, ref, ag_send.at[i, k], ag_recv.at[i, k], (mate, plus, minus)[k])

    def fwd_copy(r, k):
        i = kv_round if r is None else r
        owner, lines = ((minus, everything), (plus, everything), (plus2, top), (plus2, bottom))[k]
        ref = block(r, owner, lines)
        return remote(ref, ref, fwd_send.at[i, k], fwd_recv.at[i, k], mate)

    def fwd_recv_copy(r, k):
        i = kv_round if r is None else r
        flip = 1 - 2 * core
        owner, lines = ((minus, everything), (plus, everything), (plus2, top), (plus2, bottom))[k]
        ref = block(r, owner + flip, lines)
        return remote(ref, ref, fwd_send.at[i, k], fwd_recv.at[i, k], mate)

    for j in range(4):
        slab(0, j).start()
    own_kv = pltpu.make_async_copy(kv_ref, kvs_ref.at[:, pl.ds(pl.multiple_of(me * nk, nk), nk)], kv_sem)
    own_kv.start()

    barrier = pltpu.get_barrier_semaphore()
    for to in (mate, plus, minus):
        pl.semaphore_signal(barrier, inc=1, device_id={"model": to}, device_id_type=MESH)

    @pl.loop(0, ROUNDS)
    def _(r):
        own_x(r).start()

    own_kv.wait()
    pl.semaphore_wait(barrier, 3)
    for k in range(3):
        gather_copy(None, k).start()

    def pair_sum(r, j):
        pair_copy(r, j).wait_recv()
        part[r, j, core] = part[r, j, core] + pair[r, j]
        if j == 0:
            for way in range(2):
                hop_copy(r, way).start()
        elif j < 3:
            near_copy(r, j - 1, False).start()

    def add_hops(r):
        for way in range(2):
            hop_copy(r, way).wait_recv()
            lines = (top, bottom)[way]
            part[r, 1 + way, core, lines] = part[r, 1 + way, core, lines] + hop[r, way]
            near_copy(r, way, True).start()

    def relay(r):
        for way in range(2):
            received(r, 1 + way).wait_recv()
            relay_copy(r, way).start()
            fwd_copy(r, way).start()

    def pass_far(r):
        for way in range(2):
            relayed_recv(r, way).wait_recv()
            fwd_copy(r, 2 + way).start()

    @pl.loop(0, ROUNDS)
    def _(r):
        for j in range(4):
            slab(r, j).wait()
            product = jnp.dot(o_ref[...], wbuf[j], preferred_element_type=F32)
            for q in range(CORES):
                part[r, j, q] = product[:, q * n:(q + 1) * n]
            pair_copy(r, j).start()

            @pl.when(r < ROUNDS - 1)
            def _():
                slab(r + 1, j).start()

            if j >= 2:
                pair_sum(r, j - 2)
            else:
                @pl.when(r >= 1)
                def _():
                    pair_sum(r - 1, j + 2)

        @pl.when(r == 0)
        def _():
            relay(None)

        @pl.when(r == 2)
        def _():
            pass_far(None)

        @pl.when(r >= 2)
        def _():
            add_hops(r - 2)

    for j in (2, 3):
        pair_sum(ROUNDS - 1, j)
    for r in (ROUNDS - 2, ROUNDS - 1):
        add_hops(r)

    def finish(r):
        for way in range(2):
            for late in (False, True):
                near_copy(r, way, late).wait_recv()
        own_x(r).wait()
        total = part[r, 3, core] + (near[r, 0] + near[r, 1])
        total = xbuf[r].astype(F32) + total
        y_ref[:, pl.ds(pl.multiple_of(r * width + me * n, n), n)] = total.astype(BF16)
        for k in range(3):
            gather_copy(r, k).start()

    @pl.loop(0, ROUNDS + 4)
    def _(i):
        @pl.when(i < ROUNDS)
        def _():
            finish(i)

        @pl.when((i >= 2) & (i < ROUNDS + 2))
        def _():
            relay(i - 2)

        @pl.when(i >= 4)
        def _():
            pass_far(i - 4)

    def drain(r):
        received(r, 0).wait_recv()
        for k in range(4):
            fwd_recv_copy(r, k).wait_recv()
        for k in range(3):
            gather_copy(r, k).wait_send()
        for way in range(2):
            relay_copy(r, way).wait_send()
        for k in range(4):
            fwd_copy(r, k).wait_send()

    @pl.loop(0, ROUNDS)
    def _(r):
        for j in range(4):
            pair_copy(r, j).wait_send()
        for way in range(2):
            hop_copy(r, way).wait_send()
            for late in (False, True):
                near_copy(r, way, late).wait_send()
        drain(r)

    drain(None)


def out_product(size, o, kv, x, w_out):
    rows, depth = o.shape
    model = w_out.shape[1]
    n = model // (ROUNDS * size)
    sem = pltpu.SemaphoreType.DMA
    return pl.pallas_call(
        functools.partial(out_kernel, size),
        out_shape=(pltpu.VMEM((rows, model), BF16), pltpu.VMEM((rows, size * kv.shape[1]), BF16)),
        in_specs=[
            pl.BlockSpec(memory_space=pltpu.VMEM),
            pl.BlockSpec(memory_space=pl.ANY),
            pl.BlockSpec(memory_space=pl.ANY),
            pl.BlockSpec(memory_space=pl.ANY),
        ],
        out_specs=(pl.BlockSpec(memory_space=pltpu.VMEM), pl.BlockSpec(memory_space=pltpu.VMEM)),
        scratch_shapes=[
            pltpu.VMEM((4, depth, CORES * n), BF16),
            pltpu.VMEM((ROUNDS, rows, n), BF16),
            pltpu.VMEM((ROUNDS, 4, CORES, rows, n), F32),
            pltpu.VMEM((ROUNDS, 4, rows, n), F32),
            pltpu.VMEM((ROUNDS, 2, rows // 2, n), F32),
            pltpu.VMEM((ROUNDS, 2, rows, n), F32),
            sem((4,)), sem((ROUNDS,)), sem,
            sem((ROUNDS, 4)), sem((ROUNDS, 4)),
            sem((ROUNDS, 2)), sem((ROUNDS, 2)),
            sem((ROUNDS, 4)), sem((ROUNDS, 4)),
            sem((ROUNDS + 1, 5)), sem((ROUNDS + 1, 5)),
            sem((ROUNDS + 1, 4)), sem((ROUNDS + 1, 4)),
        ],
        compiler_params=pltpu.CompilerParams(
            collective_id=0, has_side_effects=True, vmem_limit_bytes=48 * 1024 * 1024),
        cost_estimate=pl.CostEstimate(
            flops=2 * rows * depth * model, bytes_accessed=depth * model * 2, transcendentals=0),
        name="out_reduce",
    )(o, kv, x, w_out)


def solution(mesh):
    size = mesh.shape["model"]

    def local_step(x, w_query, w_key, w_value, w_out, k_cache, v_cache, lengths):
        rows = x.shape[0]
        head_dim = k_cache.shape[3]
        kv_heads = k_cache.shape[1]
        me = lax.axis_index("model")
        q = jnp.dot(x, w_query, preferred_element_type=F32).astype(BF16)
        wk = lax.dynamic_slice_in_dim(w_key, me * head_dim, head_dim, axis=1)
        wv = lax.dynamic_slice_in_dim(w_value, me * head_dim, head_dim, axis=1)
        k_one = jnp.dot(x, wk, preferred_element_type=F32).astype(BF16)
        v_one = jnp.dot(x, wv, preferred_element_type=F32).astype(BF16)
        out = attend(
            q.reshape(rows, -1, head_dim),
            lax.dynamic_index_in_dim(k_cache, me, axis=1, keepdims=False),
            lax.dynamic_index_in_dim(v_cache, me, axis=1, keepdims=False),
            k_one, v_one, lengths)
        kv = jnp.concatenate([k_one, v_one], axis=1)
        y, kvs = out_product(size, out.reshape(rows, -1), kv, x, w_out)
        kvs = kvs.reshape(rows, kv_heads, 2, head_dim)
        return y, kvs[:, :, 0], kvs[:, :, 1]

    rows_spec = P("replica")
    return jax.shard_map(
        local_step,
        mesh=mesh,
        in_specs=(P("replica", None), P(None, "model"), P(), P(), P("model", None), rows_spec, rows_spec, rows_spec),
        out_specs=(rows_spec, rows_spec, rows_spec),
        check_vma=False,
    )
```

```python
import functools

import jax
import jax.numpy as jnp
from jax import lax
from jax.experimental import pallas as pl
from jax.experimental.pallas import tpu as pltpu
from jax.sharding import PartitionSpec as P

MESH = pl.DeviceIdType.MESH
CORES = 2
ROUNDS = 8
DEPTH = 512
SHORT = 32
LONG_STEP = 4
OFFSETS = (2, 1, 3, 0)
BF16 = jnp.bfloat16
F32 = jnp.float32


def front_kernel(x_ref, wq_ref, wk_ref, wv_ref, kc_ref, vc_ref, len_ref, o_ref, kv_ref,
                 xbuf, wbuf, acc, qbuf, obuf, kshort, vshort, klong, vlong, lens, order,
                 x_sem, w_sem, short_sem, long_sem, len_sem):
    me = lax.axis_index("model")
    steps, rows, depth = xbuf.shape
    slots = wbuf.shape[0]
    heads, dim = qbuf.shape[1:]
    width = heads * dim
    context = klong.shape[1]
    unit = context // SHORT
    per_step = rows // steps
    head_cols = pl.ds(pl.multiple_of(me * dim, dim), dim)

    def x_copy(s):
        cols = pl.ds(pl.multiple_of(s * depth, depth), depth)
        return pltpu.make_async_copy(x_ref.at[:, cols], xbuf.at[s], x_sem.at[s])

    def w_copies(s, slot):
        lines = pl.ds(pl.multiple_of(s * depth, depth), depth)
        return (
            pltpu.make_async_copy(wq_ref.at[lines], wbuf.at[slot, :, pl.ds(0, width)], w_sem.at[slot, 0]),
            pltpu.make_async_copy(wk_ref.at[lines, head_cols], wbuf.at[slot, :, pl.ds(width, dim)], w_sem.at[slot, 1]),
            pltpu.make_async_copy(wv_ref.at[lines, head_cols], wbuf.at[slot, :, pl.ds(width + dim, dim)], w_sem.at[slot, 2]),
        )

    def short_copies():
        lines = pl.ds(0, SHORT)
        return (pltpu.make_async_copy(kc_ref.at[:, me, lines], kshort, short_sem.at[0]),
                pltpu.make_async_copy(vc_ref.at[:, me, lines], vshort, short_sem.at[1]))

    def long_copies(b, slot):
        return (pltpu.make_async_copy(kc_ref.at[b, me], klong.at[slot], long_sem.at[0]),
                pltpu.make_async_copy(vc_ref.at[b, me], vlong.at[slot], long_sem.at[1]))

    len_copy = pltpu.make_async_copy(len_ref, lens, len_sem)
    for s in range(slots):
        x_copy(s).start()
        for copy in w_copies(s, s):
            copy.start()
        if s == 0:
            len_copy.start()

    @pl.loop(slots, steps)
    def _(s):
        x_copy(s).start()

    acc[...] = jnp.zeros_like(acc)
    len_copy.wait()

    def stream(s, count):
        slot = lax.rem(s, slots)
        x_copy(s).wait()
        for copy in w_copies(s, slot):
            copy.wait()
        acc[...] += jnp.dot(xbuf[s], wbuf[slot], preferred_element_type=F32)

        @pl.when(s + slots < steps)
        def _():
            for copy in w_copies(s + slots, slot):
                copy.start()

        @pl.when(s == steps // 4)
        def _():
            for copy in short_copies():
                copy.start()

        for i in range(per_step):
            b = s * per_step + i
            is_long = lens[b] > SHORT

            @pl.when(is_long)
            def _():
                order[count] = b
                for copy in long_copies(b, count):
                    copy.start()

            count = count + is_long.astype(jnp.int32)
        return count

    count = lax.fori_loop(0, steps, stream, jnp.int32(0))

    for h in range(heads):
        qbuf[:, h, :] = acc[:, h * dim:(h + 1) * dim].astype(BF16).astype(F32)
    kv_ref[...] = acc[:, width:].astype(BF16)
    for copy in short_copies():
        copy.wait()

    inv_sqrt = dim ** -0.5
    contract_last = (((1,), (1,)), ((), ()))

    def attend(q, keys, values, valid, valid_new):
        scores = lax.dot_general(q, keys, contract_last, preferred_element_type=F32) * inv_sqrt
        score_new = lax.dot_general(q, kv_ref[:, :dim], contract_last, preferred_element_type=F32) * inv_sqrt
        scores = jnp.where(valid, scores, -jnp.inf)
        score_new = jnp.where(valid_new, score_new, -jnp.inf)
        row_max = jnp.maximum(jnp.max(scores, axis=-1, keepdims=True), jnp.max(score_new, axis=-1, keepdims=True))
        weights = jnp.exp(scores - row_max)
        weight_new = jnp.exp(score_new - row_max)
        norm = jnp.sum(weights, axis=-1, keepdims=True) + jnp.sum(weight_new, axis=-1, keepdims=True)
        total = jnp.dot(weights.astype(BF16), values, preferred_element_type=F32)
        total = total + jnp.dot(weight_new.astype(BF16), kv_ref[:, dim:], preferred_element_type=F32)
        return total / norm

    def iota(shape, axis):
        return lax.broadcasted_iota(jnp.int32, shape, axis)

    short_rows = unit * heads
    row_seq = iota((short_rows, 1), 0) // heads
    col = iota((short_rows, context), 1)
    place = jnp.where(col // SHORT == row_seq, col % SHORT, context)
    new_seq = iota((short_rows, rows), 1) - row_seq
    line = iota((1, context), 1)

    @pl.loop(0, rows // unit // 2)
    def _(pair):
        for i in range(2):
            first = (pair * 2 + i) * unit
            bound = jnp.zeros((1, context), jnp.int32)
            for j in range(unit):
                bound = jnp.where(line // SHORT == j, lens[first + j], bound)
            seqs = pl.ds(pl.multiple_of(first, unit), unit)
            out = attend(
                qbuf[seqs].reshape(short_rows, dim).astype(BF16),
                kshort[seqs].reshape(context, dim), vshort[seqs].reshape(context, dim),
                place < bound, new_seq == first)
            obuf[seqs] = out.reshape(unit, heads, dim)

    @pl.loop(0, count)
    def _(i):
        for copy in long_copies(0, 0):
            copy.wait()

    long_col = iota((heads, context), 1)
    long_seq = iota((heads, rows), 1)

    @pl.loop(0, (count + LONG_STEP - 1) // LONG_STEP)
    def _(i):
        for j in range(LONG_STEP):
            slot = jnp.minimum(i * LONG_STEP + j, count - 1)
            b = order[slot]
            obuf[b] = attend(
                qbuf[b].astype(BF16), klong[slot], vlong[slot], long_col < lens[b], long_seq == b)

    for h in range(heads):
        o_ref[:, h * dim:(h + 1) * dim] = obuf[:, h, :].astype(BF16)


def front(x, w_query, w_key, w_value, k_cache, v_cache, lengths):
    rows, model = x.shape
    width = w_query.shape[1]
    context, dim = k_cache.shape[2:]
    heads = width // dim
    steps = model // DEPTH
    sem = pltpu.SemaphoreType.DMA
    total = width + 2 * dim
    return pl.pallas_call(
        front_kernel,
        out_shape=(pltpu.VMEM((rows, width), BF16), pltpu.VMEM((rows, 2 * dim), BF16)),
        in_specs=[pl.BlockSpec(memory_space=pl.ANY)] * 7,
        out_specs=(pl.BlockSpec(memory_space=pltpu.VMEM), pl.BlockSpec(memory_space=pltpu.VMEM)),
        scratch_shapes=[
            pltpu.VMEM((steps, rows, DEPTH), BF16),
            pltpu.VMEM((4, DEPTH, total), BF16),
            pltpu.VMEM((rows, total), F32),
            pltpu.VMEM((rows, heads, dim), F32),
            pltpu.VMEM((rows, heads, dim), F32),
            pltpu.VMEM((rows, SHORT, dim), BF16),
            pltpu.VMEM((rows, SHORT, dim), BF16),
            pltpu.VMEM((rows, context, dim), BF16),
            pltpu.VMEM((rows, context, dim), BF16),
            pltpu.SMEM((rows,), jnp.int32),
            pltpu.SMEM((rows,), jnp.int32),
            sem((steps,)), sem((4, 3)), sem((2,)), sem((2,)), sem,
        ],
        compiler_params=pltpu.CompilerParams(vmem_limit_bytes=52 * 1024 * 1024),
        cost_estimate=pl.CostEstimate(
            flops=2 * rows * model * total, bytes_accessed=model * total * 2, transcendentals=0),
        name="front",
    )(x, w_query, w_key, w_value, k_cache, v_cache, lengths)


def out_kernel(size, o_ref, kv_ref, x_ref, w_ref, y_ref, kvs_ref,
               wbuf, xbuf, part, pair, hop, near,
               w_sem, x_sem, kv_sem, pair_send, pair_recv, hop_send, hop_recv, near_send, near_recv,
               ag_send, ag_recv, fwd_send, fwd_recv):
    me = lax.axis_index("model")
    core = lax.rem(me, CORES)
    chip = me // CORES
    chips = size // CORES
    plus = lax.rem(me + CORES, size)
    minus = lax.rem(me + size - CORES, size)
    mate = me + 1 - 2 * core
    plus2 = lax.rem(me + 2 * CORES, size)
    rows, depth = o_ref.shape
    half = rows // 2
    n, nk = part.shape[-1], kv_ref.shape[1]
    width = n * size
    top, bottom = pl.ds(0, half), pl.ds(half, half)
    kv_round = ROUNDS

    def slab(r, j):
        dest = lax.rem(chip + OFFSETS[j], chips)
        cols = pl.ds(pl.multiple_of(r * width + dest * (CORES * n), CORES * n), CORES * n)
        return pltpu.make_async_copy(w_ref.at[:, cols], wbuf.at[j], w_sem.at[j])

    def own_x(r):
        cols = pl.ds(pl.multiple_of(r * width + me * n, n), n)
        return pltpu.make_async_copy(x_ref.at[:, cols], xbuf.at[r], x_sem.at[r])

    def remote(src, dst, send, recv, to):
        return pltpu.make_async_remote_copy(
            src_ref=src, dst_ref=dst, send_sem=send, recv_sem=recv,
            device_id={"model": to}, device_id_type=MESH)

    def pair_copy(r, j):
        return remote(part.at[r, j, 1 - core], pair.at[r, j], pair_send.at[r, j], pair_recv.at[r, j], mate)

    def hop_copy(r, way):
        to, lines = ((plus, top), (minus, bottom))[way]
        return remote(part.at[r, 0, core, lines], hop.at[r, way], hop_send.at[r, way], hop_recv.at[r, way], to)

    def near_copy(r, way, late):
        to = (plus, minus)[way]
        lines = top if (way == 0) == late else bottom
        k = 2 * way + int(late)
        return remote(part.at[r, 1 + way, core, lines], near.at[r, way, lines],
                      near_send.at[r, k], near_recv.at[r, k], to)

    def block(r, owner, lines):
        if r is None:
            return kvs_ref.at[lines, pl.ds(pl.multiple_of(owner * nk, nk), nk)]
        return y_ref.at[lines, pl.ds(pl.multiple_of(r * width + owner * n, n), n)]

    everything = pl.ds(0, rows)

    def gather_copy(r, k):
        i = kv_round if r is None else r
        ref = block(r, me, everything)
        return remote(ref, ref, ag_send.at[i, k], ag_recv.at[i, k], (mate, plus, minus)[k])

    def relay_copy(r, way):
        i = kv_round if r is None else r
        ref = block(r, (minus, plus)[way], (top, bottom)[way])
        return remote(ref, ref, ag_send.at[i, 3 + way], ag_recv.at[i, 3 + way], (plus, minus)[way])

    def relayed_recv(r, way):
        i = kv_round if r is None else r
        ref = block(r, plus2, (top, bottom)[way])
        return remote(ref, ref, ag_send.at[i, 3 + way], ag_recv.at[i, 3 + way], (plus, minus)[way])

    def received(r, k):
        i = kv_round if r is None else r
        ref = block(r, (mate, minus, plus)[k], everything)
        return remote(ref, ref, ag_send.at[i, k], ag_recv.at[i, k], (mate, plus, minus)[k])

    def fwd_copy(r, k):
        i = kv_round if r is None else r
        owner, lines = ((minus, everything), (plus, everything), (plus2, top), (plus2, bottom))[k]
        ref = block(r, owner, lines)
        return remote(ref, ref, fwd_send.at[i, k], fwd_recv.at[i, k], mate)

    def fwd_recv_copy(r, k):
        i = kv_round if r is None else r
        flip = 1 - 2 * core
        owner, lines = ((minus, everything), (plus, everything), (plus2, top), (plus2, bottom))[k]
        ref = block(r, owner + flip, lines)
        return remote(ref, ref, fwd_send.at[i, k], fwd_recv.at[i, k], mate)

    for j in range(4):
        slab(0, j).start()
    own_kv = pltpu.make_async_copy(kv_ref, kvs_ref.at[:, pl.ds(pl.multiple_of(me * nk, nk), nk)], kv_sem)
    own_kv.start()

    barrier = pltpu.get_barrier_semaphore()
    for to in (mate, plus, minus):
        pl.semaphore_signal(barrier, inc=1, device_id={"model": to}, device_id_type=MESH)

    @pl.loop(0, ROUNDS)
    def _(r):
        own_x(r).start()

    own_kv.wait()
    pl.semaphore_wait(barrier, 3)
    for k in range(3):
        gather_copy(None, k).start()

    def pair_sum(r, j):
        pair_copy(r, j).wait_recv()
        part[r, j, core] = part[r, j, core] + pair[r, j]
        if j == 0:
            for way in range(2):
                hop_copy(r, way).start()
        elif j < 3:
            near_copy(r, j - 1, False).start()

    def add_hops(r):
        for way in range(2):
            hop_copy(r, way).wait_recv()
            lines = (top, bottom)[way]
            part[r, 1 + way, core, lines] = part[r, 1 + way, core, lines] + hop[r, way]
            near_copy(r, way, True).start()

    def relay(r):
        for way in range(2):
            received(r, 1 + way).wait_recv()
            relay_copy(r, way).start()
            fwd_copy(r, way).start()

    def pass_far(r):
        for way in range(2):
            relayed_recv(r, way).wait_recv()
            fwd_copy(r, 2 + way).start()

    @pl.loop(0, ROUNDS)
    def _(r):
        for j in range(4):
            slab(r, j).wait()
            product = jnp.dot(o_ref[...], wbuf[j], preferred_element_type=F32)
            for q in range(CORES):
                part[r, j, q] = product[:, q * n:(q + 1) * n]
            pair_copy(r, j).start()

            @pl.when(r < ROUNDS - 1)
            def _():
                slab(r + 1, j).start()

            if j >= 2:
                pair_sum(r, j - 2)
            else:
                @pl.when(r >= 1)
                def _():
                    pair_sum(r - 1, j + 2)

        @pl.when(r == 0)
        def _():
            relay(None)

        @pl.when(r == 2)
        def _():
            pass_far(None)

        @pl.when(r >= 2)
        def _():
            add_hops(r - 2)

    for j in (2, 3):
        pair_sum(ROUNDS - 1, j)
    for r in (ROUNDS - 2, ROUNDS - 1):
        add_hops(r)

    def finish(r):
        for way in range(2):
            for late in (False, True):
                near_copy(r, way, late).wait_recv()
        own_x(r).wait()
        total = part[r, 3, core] + (near[r, 0] + near[r, 1])
        total = xbuf[r].astype(F32) + total
        y_ref[:, pl.ds(pl.multiple_of(r * width + me * n, n), n)] = total.astype(BF16)
        for k in range(3):
            gather_copy(r, k).start()

    @pl.loop(0, ROUNDS + 4)
    def _(i):
        @pl.when(i < ROUNDS)
        def _():
            finish(i)

        @pl.when((i >= 2) & (i < ROUNDS + 2))
        def _():
            relay(i - 2)

        @pl.when(i >= 4)
        def _():
            pass_far(i - 4)

    def drain(r):
        received(r, 0).wait_recv()
        for k in range(4):
            fwd_recv_copy(r, k).wait_recv()
        for k in range(3):
            gather_copy(r, k).wait_send()
        for way in range(2):
            relay_copy(r, way).wait_send()
        for k in range(4):
            fwd_copy(r, k).wait_send()

    @pl.loop(0, ROUNDS)
    def _(r):
        for j in range(4):
            pair_copy(r, j).wait_send()
        for way in range(2):
            hop_copy(r, way).wait_send()
            for late in (False, True):
                near_copy(r, way, late).wait_send()
        drain(r)

    drain(None)


def out_product(size, o, kv, x, w_out):
    rows, depth = o.shape
    model = w_out.shape[1]
    n = model // (ROUNDS * size)
    sem = pltpu.SemaphoreType.DMA
    return pl.pallas_call(
        functools.partial(out_kernel, size),
        out_shape=(pltpu.VMEM((rows, model), BF16), pltpu.VMEM((rows, size * kv.shape[1]), BF16)),
        in_specs=[
            pl.BlockSpec(memory_space=pltpu.VMEM),
            pl.BlockSpec(memory_space=pl.ANY),
            pl.BlockSpec(memory_space=pl.ANY),
            pl.BlockSpec(memory_space=pl.ANY),
        ],
        out_specs=(pl.BlockSpec(memory_space=pltpu.VMEM), pl.BlockSpec(memory_space=pltpu.VMEM)),
        scratch_shapes=[
            pltpu.VMEM((4, depth, CORES * n), BF16),
            pltpu.VMEM((ROUNDS, rows, n), BF16),
            pltpu.VMEM((ROUNDS, 4, CORES, rows, n), F32),
            pltpu.VMEM((ROUNDS, 4, rows, n), F32),
            pltpu.VMEM((ROUNDS, 2, rows // 2, n), F32),
            pltpu.VMEM((ROUNDS, 2, rows, n), F32),
            sem((4,)), sem((ROUNDS,)), sem,
            sem((ROUNDS, 4)), sem((ROUNDS, 4)),
            sem((ROUNDS, 2)), sem((ROUNDS, 2)),
            sem((ROUNDS, 4)), sem((ROUNDS, 4)),
            sem((ROUNDS + 1, 5)), sem((ROUNDS + 1, 5)),
            sem((ROUNDS + 1, 4)), sem((ROUNDS + 1, 4)),
        ],
        compiler_params=pltpu.CompilerParams(
            collective_id=0, has_side_effects=True, vmem_limit_bytes=48 * 1024 * 1024),
        cost_estimate=pl.CostEstimate(
            flops=2 * rows * depth * model, bytes_accessed=depth * model * 2, transcendentals=0),
        name="out_reduce",
    )(o, kv, x, w_out)


def solution(mesh):
    size = mesh.shape["model"]

    def local_step(x, w_query, w_key, w_value, w_out, k_cache, v_cache, lengths):
        rows = x.shape[0]
        head_dim = k_cache.shape[3]
        kv_heads = k_cache.shape[1]
        out, kv = front(x, w_query, w_key, w_value, k_cache, v_cache, lengths)
        y, kvs = out_product(size, out, kv, x, w_out)
        kvs = kvs.reshape(rows, kv_heads, 2, head_dim)
        return y, kvs[:, :, 0], kvs[:, :, 1]

    rows_spec = P("replica")
    return jax.shard_map(
        local_step,
        mesh=mesh,
        in_specs=(P("replica", None), P(None, "model"), P(), P(), P("model", None), rows_spec, rows_spec, rows_spec),
        out_specs=(rows_spec, rows_spec, rows_spec),
        check_vma=False,
    )
```

```python
import functools

import jax
import jax.numpy as jnp
from jax import lax
from jax.experimental import pallas as pl
from jax.experimental.pallas import tpu as pltpu
from jax.sharding import PartitionSpec as P

MESH = pl.DeviceIdType.MESH
CORES = 2
ROUNDS = 8
WRITES = 8
DEPTH = 512
SHORT = 32
SHORT_STEP = 4
PACK = 16
LONG_STEP = 10
OFFSETS = (2, 1, 3, 0)
BF16 = jnp.bfloat16
F32 = jnp.float32


def front_kernel(x_ref, wq_ref, wk_ref, wv_ref, kc_ref, vc_ref, len_ref, o_ref, kv_ref,
                 xbuf, wbuf, acc, kvf, qbuf, obuf, kshort, vshort, klong, vlong, lens, order,
                 x_sem, w_sem, short_sem, long_sem, len_sem):
    me = lax.axis_index("model")
    steps, rows, depth = xbuf.shape
    slots = wbuf.shape[0]
    heads, dim = qbuf.shape[1:]
    width = heads * dim
    context = klong.shape[1]
    unit = context // SHORT
    per_step = rows // steps
    head_cols = pl.ds(pl.multiple_of(me * dim, dim), dim)

    def x_copy(s):
        cols = pl.ds(pl.multiple_of(s * depth, depth), depth)
        return pltpu.make_async_copy(x_ref.at[:, cols], xbuf.at[s], x_sem.at[s])

    def w_copies(s, slot):
        lines = pl.ds(pl.multiple_of(s * depth, depth), depth)
        return (
            pltpu.make_async_copy(wq_ref.at[lines], wbuf.at[slot, :, pl.ds(0, width)], w_sem.at[slot, 0]),
            pltpu.make_async_copy(wk_ref.at[lines, head_cols], wbuf.at[slot, :, pl.ds(width, dim)], w_sem.at[slot, 1]),
            pltpu.make_async_copy(wv_ref.at[lines, head_cols], wbuf.at[slot, :, pl.ds(width + dim, dim)], w_sem.at[slot, 2]),
        )

    def short_copies():
        lines = pl.ds(0, SHORT)
        return (pltpu.make_async_copy(kc_ref.at[:, me, lines], kshort, short_sem.at[0]),
                pltpu.make_async_copy(vc_ref.at[:, me, lines], vshort, short_sem.at[1]))

    def long_copies(b, slot):
        return (pltpu.make_async_copy(kc_ref.at[b, me], klong.at[slot], long_sem.at[0]),
                pltpu.make_async_copy(vc_ref.at[b, me], vlong.at[slot], long_sem.at[1]))

    len_copy = pltpu.make_async_copy(len_ref, lens, len_sem)
    for s in range(slots):
        x_copy(s).start()
        for copy in w_copies(s, s):
            copy.start()
        if s == 0:
            len_copy.start()

    @pl.loop(slots, steps)
    def _(s):
        x_copy(s).start()

    acc[...] = jnp.zeros_like(acc)
    len_copy.wait()

    def stream(s, count):
        slot = lax.rem(s, slots)
        x_copy(s).wait()
        for copy in w_copies(s, slot):
            copy.wait()
        acc[...] += jnp.dot(xbuf[s], wbuf[slot], preferred_element_type=F32)

        @pl.when(s + slots < steps)
        def _():
            for copy in w_copies(s + slots, slot):
                copy.start()

        @pl.when(s == steps // 4)
        def _():
            for copy in short_copies():
                copy.start()

        for i in range(per_step):
            b = s * per_step + i
            is_long = lens[b] > SHORT - 1

            @pl.when(is_long)
            def _():
                order[count] = b
                for copy in long_copies(b, count):
                    copy.start()

            count = count + is_long.astype(jnp.int32)
        return count

    count = lax.fori_loop(0, steps, stream, jnp.int32(0))

    kv = acc[:, width:].astype(BF16)
    kv_ref[...] = kv
    kvf[...] = kv.astype(F32)
    for h in range(heads):
        qbuf[:, h, :] = acc[:, h * dim:(h + 1) * dim].astype(BF16).astype(F32)

    inv_sqrt = dim ** -0.5
    contract_last = (((1,), (1,)), ((), ()))

    def iota(shape, axis):
        return lax.broadcasted_iota(jnp.int32, shape, axis)

    is_last = iota((PACK, dim), 0) == PACK - 1

    def put_new(keys, values, slot, size, b):
        lines = pl.ds(size - PACK, PACK)
        row = kvf[pl.ds(b, 1), :]
        new_key = jnp.broadcast_to(row[:, :dim], (PACK, dim)).astype(BF16)
        new_value = jnp.broadcast_to(row[:, dim:], (PACK, dim)).astype(BF16)
        keys[slot, lines, :] = jnp.where(is_last, new_key, keys[slot, lines, :])
        values[slot, lines, :] = jnp.where(is_last, new_value, values[slot, lines, :])

    def attend(items):
        scores = [lax.dot_general(q, keys, contract_last, preferred_element_type=F32) for q, keys, _, _ in items]
        weights, norms = [], []
        for score, (_, _, _, valid) in zip(scores, items):
            score = jnp.where(valid, score * inv_sqrt, -jnp.inf)
            weight = jnp.exp(score - jnp.max(score, axis=-1, keepdims=True))
            norms.append(jnp.sum(weight, axis=-1, keepdims=True))
            weights.append(weight.astype(BF16))
        totals = [jnp.dot(weight, item[2], preferred_element_type=F32) for weight, item in zip(weights, items)]
        return [total / norm for total, norm in zip(totals, norms)]

    for copy in short_copies():
        copy.wait()

    @pl.loop(0, rows // unit)
    def _(u):
        for j in range(unit):
            put_new(kshort, vshort, u * unit + j, SHORT, u * unit + j)

    short_rows = unit * heads
    col = iota((short_rows, context), 1)
    own = col // SHORT == iota((short_rows, 1), 0) // heads
    place = jnp.where(own, jnp.where(col % SHORT == SHORT - 1, -1, col % SHORT), context)
    line = iota((1, context), 1)

    @pl.loop(0, rows // unit // SHORT_STEP)
    def _(group):
        items, places = [], []
        for i in range(SHORT_STEP):
            first = (group * SHORT_STEP + i) * unit
            bound = jnp.zeros((1, context), jnp.int32)
            for j in range(unit):
                bound = jnp.where(line // SHORT == j, lens[first + j], bound)
            seqs = pl.ds(pl.multiple_of(first, unit), unit)
            places.append(seqs)
            items.append((
                qbuf[seqs].reshape(short_rows, dim).astype(BF16),
                kshort[seqs].reshape(context, dim), vshort[seqs].reshape(context, dim), place < bound))
        for seqs, out in zip(places, attend(items)):
            obuf[seqs] = out.reshape(unit, heads, dim)

    @pl.loop(0, count)
    def _(i):
        for copy in long_copies(0, 0):
            copy.wait()

    @pl.loop(0, count)
    def _(i):
        put_new(klong, vlong, i, context, order[i])

    long_col = iota((heads, context), 1)
    long_place = jnp.where(long_col == context - 1, -1, long_col)

    @pl.loop(0, (count + LONG_STEP - 1) // LONG_STEP)
    def _(i):
        slots = [jnp.minimum(i * LONG_STEP + j, count - 1) for j in range(LONG_STEP)]
        seqs = [order[slot] for slot in slots]
        outs = attend([(qbuf[b].astype(BF16), klong[slot], vlong[slot], long_place < lens[b])
                       for slot, b in zip(slots, seqs)])
        for b, out in zip(seqs, outs):
            obuf[b] = out

    for h in range(heads):
        o_ref[:, h * dim:(h + 1) * dim] = obuf[:, h, :].astype(BF16)


def front(x, w_query, w_key, w_value, k_cache, v_cache, lengths):
    rows, model = x.shape
    width = w_query.shape[1]
    context, dim = k_cache.shape[2:]
    heads = width // dim
    steps = model // DEPTH
    sem = pltpu.SemaphoreType.DMA
    total = width + 2 * dim
    return pl.pallas_call(
        front_kernel,
        out_shape=(pltpu.VMEM((rows, width), BF16), pltpu.VMEM((rows, 2 * dim), BF16)),
        in_specs=[pl.BlockSpec(memory_space=pl.ANY)] * 6 + [pl.BlockSpec(memory_space=pltpu.HBM)],
        out_specs=(pl.BlockSpec(memory_space=pltpu.VMEM), pl.BlockSpec(memory_space=pltpu.VMEM)),
        scratch_shapes=[
            pltpu.VMEM((steps, rows, DEPTH), BF16),
            pltpu.VMEM((4, DEPTH, total), BF16),
            pltpu.VMEM((rows, total), F32),
            pltpu.VMEM((rows, 2 * dim), F32),
            pltpu.VMEM((rows, heads, dim), F32),
            pltpu.VMEM((rows, heads, dim), F32),
            pltpu.VMEM((rows, SHORT, dim), BF16),
            pltpu.VMEM((rows, SHORT, dim), BF16),
            pltpu.VMEM((rows, context, dim), BF16),
            pltpu.VMEM((rows, context, dim), BF16),
            pltpu.SMEM((rows,), jnp.int32),
            pltpu.SMEM((rows,), jnp.int32),
            sem((steps,)), sem((4, 3)), sem((2,)), sem((2,)), sem,
        ],
        compiler_params=pltpu.CompilerParams(vmem_limit_bytes=52 * 1024 * 1024),
        cost_estimate=pl.CostEstimate(
            flops=2 * rows * model * total, bytes_accessed=model * total * 2, transcendentals=0),
        name="front",
    )(x, w_query, w_key, w_value, k_cache, v_cache, lengths)


def out_kernel(size, o_ref, kv_ref, x_ref, w_ref, y_ref, k_ref, v_ref,
               kvs_ref, kv_heads, wbuf, xbuf, part, pair, hop, near,
               w_sem, x_sem, kv_sem, pair_send, pair_recv, hop_send, hop_recv, near_send, near_recv,
               ag_send, ag_recv, fwd_send, fwd_recv):
    me = lax.axis_index("model")
    core = lax.rem(me, CORES)
    chip = me // CORES
    chips = size // CORES
    plus = lax.rem(me + CORES, size)
    minus = lax.rem(me + size - CORES, size)
    mate = me + 1 - 2 * core
    plus2 = lax.rem(me + 2 * CORES, size)
    rows, depth = o_ref.shape
    half = rows // 2
    n, nk = part.shape[-1], kv_ref.shape[1]
    width = n * size
    top, bottom = pl.ds(0, half), pl.ds(half, half)
    kv_round = ROUNDS

    def slab(r, j):
        dest = lax.rem(chip + OFFSETS[j], chips)
        cols = pl.ds(pl.multiple_of(r * width + dest * (CORES * n), CORES * n), CORES * n)
        return pltpu.make_async_copy(w_ref.at[:, cols], wbuf.at[j], w_sem.at[j])

    def own_x(r):
        cols = pl.ds(pl.multiple_of(r * width + me * n, n), n)
        return pltpu.make_async_copy(x_ref.at[:, cols], xbuf.at[r], x_sem.at[r])

    def remote(src, dst, send, recv, to):
        return pltpu.make_async_remote_copy(
            src_ref=src, dst_ref=dst, send_sem=send, recv_sem=recv,
            device_id={"model": to}, device_id_type=MESH)

    def pair_copy(r, j):
        return remote(part.at[r, j, 1 - core], pair.at[r, j], pair_send.at[r, j], pair_recv.at[r, j], mate)

    def hop_copy(r, way):
        to, lines = ((plus, top), (minus, bottom))[way]
        return remote(part.at[r, 0, core, lines], hop.at[r, way], hop_send.at[r, way], hop_recv.at[r, way], to)

    def near_copy(r, way, late):
        to = (plus, minus)[way]
        lines = top if (way == 0) == late else bottom
        k = 2 * way + int(late)
        return remote(part.at[r, 1 + way, core, lines], near.at[r, way, lines],
                      near_send.at[r, k], near_recv.at[r, k], to)

    def block(r, owner, lines):
        if r is None:
            return kvs_ref.at[lines, pl.ds(pl.multiple_of(owner * nk, nk), nk)]
        return y_ref.at[lines, pl.ds(pl.multiple_of(r * width + owner * n, n), n)]

    everything = pl.ds(0, rows)

    def gather_copy(r, k):
        i = kv_round if r is None else r
        ref = block(r, me, everything)
        return remote(ref, ref, ag_send.at[i, k], ag_recv.at[i, k], (mate, plus, minus)[k])

    def relay_copy(r, way):
        i = kv_round if r is None else r
        ref = block(r, (minus, plus)[way], (top, bottom)[way])
        return remote(ref, ref, ag_send.at[i, 3 + way], ag_recv.at[i, 3 + way], (plus, minus)[way])

    def relayed_recv(r, way):
        i = kv_round if r is None else r
        ref = block(r, plus2, (top, bottom)[way])
        return remote(ref, ref, ag_send.at[i, 3 + way], ag_recv.at[i, 3 + way], (plus, minus)[way])

    def received(r, k):
        i = kv_round if r is None else r
        ref = block(r, (mate, minus, plus)[k], everything)
        return remote(ref, ref, ag_send.at[i, k], ag_recv.at[i, k], (mate, plus, minus)[k])

    def fwd_copy(r, k):
        i = kv_round if r is None else r
        owner, lines = ((minus, everything), (plus, everything), (plus2, top), (plus2, bottom))[k]
        ref = block(r, owner, lines)
        return remote(ref, ref, fwd_send.at[i, k], fwd_recv.at[i, k], mate)

    def fwd_recv_copy(r, k):
        i = kv_round if r is None else r
        flip = 1 - 2 * core
        owner, lines = ((minus, everything), (plus, everything), (plus2, top), (plus2, bottom))[k]
        ref = block(r, owner + flip, lines)
        return remote(ref, ref, fwd_send.at[i, k], fwd_recv.at[i, k], mate)

    for j in range(4):
        slab(0, j).start()
    own_kv = pltpu.make_async_copy(kv_ref, kvs_ref.at[:, pl.ds(pl.multiple_of(me * nk, nk), nk)], kv_sem)
    own_kv.start()

    barrier = pltpu.get_barrier_semaphore()
    for to in (mate, plus, minus):
        pl.semaphore_signal(barrier, inc=1, device_id={"model": to}, device_id_type=MESH)

    @pl.loop(0, ROUNDS)
    def _(r):
        own_x(r).start()

    own_kv.wait()
    pl.semaphore_wait(barrier, 3)
    for k in range(3):
        gather_copy(None, k).start()

    def pair_sum(r, j):
        pair_copy(r, j).wait_recv()
        part[r, j, core] = part[r, j, core] + pair[r, j]
        if j == 0:
            for way in range(2):
                hop_copy(r, way).start()
        elif j < 3:
            near_copy(r, j - 1, False).start()

    def add_hops(r):
        for way in range(2):
            hop_copy(r, way).wait_recv()
            lines = (top, bottom)[way]
            part[r, 1 + way, core, lines] = part[r, 1 + way, core, lines] + hop[r, way]
            near_copy(r, way, True).start()

    def relay(r):
        for way in range(2):
            received(r, 1 + way).wait_recv()
            relay_copy(r, way).start()
            fwd_copy(r, way).start()

    def pass_far(r):
        for way in range(2):
            relayed_recv(r, way).wait_recv()
            fwd_copy(r, 2 + way).start()

    @pl.loop(0, ROUNDS)
    def _(r):
        for j in range(4):
            slab(r, j).wait()
            product = jnp.dot(o_ref[...], wbuf[j], preferred_element_type=F32)
            for q in range(CORES):
                part[r, j, q] = product[:, q * n:(q + 1) * n]
            pair_copy(r, j).start()

            @pl.when(r < ROUNDS - 1)
            def _():
                slab(r + 1, j).start()

            if j >= 2:
                pair_sum(r, j - 2)
            else:
                @pl.when(r >= 1)
                def _():
                    pair_sum(r - 1, j + 2)

        @pl.when(r == 0)
        def _():
            relay(None)

        @pl.when(r == 2)
        def _():
            pass_far(None)

        @pl.when(r >= 2)
        def _():
            add_hops(r - 2)

    for j in (2, 3):
        pair_sum(ROUNDS - 1, j)
    for r in (ROUNDS - 2, ROUNDS - 1):
        add_hops(r)

    def drain(r):
        received(r, 0).wait_recv()
        for k in range(4):
            fwd_recv_copy(r, k).wait_recv()
        for k in range(3):
            gather_copy(r, k).wait_send()
        for way in range(2):
            relay_copy(r, way).wait_send()
        for k in range(4):
            fwd_copy(r, k).wait_send()

    drain(None)
    dim = nk // 2
    for i, ref in enumerate((k_ref, v_ref)):
        for owner in range(size):
            kv_heads[:, owner, :] = kvs_ref[:, owner * nk + i * dim:owner * nk + (i + 1) * dim].astype(F32)
        ref[...] = kv_heads[...].astype(BF16)

    def finish(r):
        for way in range(2):
            for late in (False, True):
                near_copy(r, way, late).wait_recv()
        own_x(r).wait()
        total = part[r, 3, core] + (near[r, 0] + near[r, 1])
        total = xbuf[r].astype(F32) + total
        y_ref[:, pl.ds(pl.multiple_of(r * width + me * n, n), n)] = total.astype(BF16)
        for k in range(3):
            gather_copy(r, k).start()

    @pl.loop(0, ROUNDS + 4)
    def _(i):
        @pl.when(i < ROUNDS)
        def _():
            finish(i)

        @pl.when((i >= 2) & (i < ROUNDS + 2))
        def _():
            relay(i - 2)

        @pl.when(i >= 4)
        def _():
            pass_far(i - 4)

    @pl.loop(0, ROUNDS)
    def _(r):
        for j in range(4):
            pair_copy(r, j).wait_send()
        for way in range(2):
            hop_copy(r, way).wait_send()
            for late in (False, True):
                near_copy(r, way, late).wait_send()
        drain(r)


def out_product(size, o, kv, x, w_out):
    rows, depth = o.shape
    model = w_out.shape[1]
    n = model // (ROUNDS * size)
    sem = pltpu.SemaphoreType.DMA
    return pl.pallas_call(
        functools.partial(out_kernel, size),
        out_shape=(pltpu.VMEM((rows, model), BF16),) + (pltpu.VMEM((rows, size, kv.shape[1] // 2), BF16),) * 2,
        in_specs=[
            pl.BlockSpec(memory_space=pltpu.VMEM),
            pl.BlockSpec(memory_space=pl.ANY),
            pl.BlockSpec(memory_space=pl.ANY),
            pl.BlockSpec(memory_space=pl.ANY),
        ],
        out_specs=(pl.BlockSpec(memory_space=pltpu.VMEM),) * 3,
        scratch_shapes=[
            pltpu.VMEM((rows, size * kv.shape[1]), BF16),
            pltpu.VMEM((rows, size, kv.shape[1] // 2), F32),
            pltpu.VMEM((4, depth, CORES * n), BF16),
            pltpu.VMEM((ROUNDS, rows, n), BF16),
            pltpu.VMEM((ROUNDS, 4, CORES, rows, n), F32),
            pltpu.VMEM((ROUNDS, 4, rows, n), F32),
            pltpu.VMEM((ROUNDS, 2, rows // 2, n), F32),
            pltpu.VMEM((ROUNDS, 2, rows, n), F32),
            sem((4,)), sem((ROUNDS,)), sem,
            sem((ROUNDS, 4)), sem((ROUNDS, 4)),
            sem((ROUNDS, 2)), sem((ROUNDS, 2)),
            sem((ROUNDS, 4)), sem((ROUNDS, 4)),
            sem((ROUNDS + 1, 5)), sem((ROUNDS + 1, 5)),
            sem((ROUNDS + 1, 4)), sem((ROUNDS + 1, 4)),
        ],
        compiler_params=pltpu.CompilerParams(
            collective_id=0, has_side_effects=True, vmem_limit_bytes=48 * 1024 * 1024),
        cost_estimate=pl.CostEstimate(
            flops=2 * rows * depth * model, bytes_accessed=depth * model * 2, transcendentals=0),
        name="out_reduce",
    )(o, kv, x, w_out)


def write_kernel(y_ref, k_ref, v_ref, y_out, k_out, v_out, sem):
    lines = y_ref.shape[0] // WRITES
    copies = [pltpu.make_async_copy(y_ref.at[pl.ds(i * lines, lines)], y_out.at[pl.ds(i * lines, lines)], sem.at[i])
              for i in range(WRITES)]
    copies.append(pltpu.make_async_copy(k_ref, k_out, sem.at[WRITES]))
    copies.append(pltpu.make_async_copy(v_ref, v_out, sem.at[WRITES + 1]))
    for copy in copies:
        copy.start()
    for copy in copies:
        copy.wait()


def write(*arrays):
    return pl.pallas_call(
        write_kernel,
        out_shape=tuple(jax.ShapeDtypeStruct(a.shape, a.dtype) for a in arrays),
        in_specs=[pl.BlockSpec(memory_space=pltpu.VMEM)] * 3,
        out_specs=(pl.BlockSpec(memory_space=pltpu.HBM),) * 3,
        scratch_shapes=[pltpu.SemaphoreType.DMA((WRITES + 2,))],
        compiler_params=pltpu.CompilerParams(vmem_limit_bytes=1024 * 1024),
        name="write",
    )(*arrays)


def solution(mesh):
    size = mesh.shape["model"]

    def local_step(x, w_query, w_key, w_value, w_out, k_cache, v_cache, lengths):
        lengths = pltpu.with_memory_space_constraint(lengths, pltpu.HBM)
        out, kv = front(x, w_query, w_key, w_value, k_cache, v_cache, lengths)
        return write(*out_product(size, out, kv, x, w_out))

    rows_spec = P("replica")
    return jax.shard_map(
        local_step,
        mesh=mesh,
        in_specs=(P("replica", None), P(None, "model"), P(), P(), P("model", None), rows_spec, rows_spec, rows_spec),
        out_specs=(rows_spec, rows_spec, rows_spec),
        check_vma=False,
    )
```

```python
import functools

import jax
import jax.numpy as jnp
from jax import lax
from jax.experimental import pallas as pl
from jax.experimental.pallas import tpu as pltpu
from jax.sharding import PartitionSpec as P

MESH = pl.DeviceIdType.MESH
CORES = 2
ROUNDS = 8
WRITES = 8
DEPTH = 512
SHORT = 32
SHORT_STEP = 4
PACK = 16
LONG_STEP = 10
OFFSETS = (2, 1, 3, 0)
BF16 = jnp.bfloat16
F32 = jnp.float32


def front_kernel(size, x_ref, wq_ref, wk_ref, wv_ref, kc_ref, vc_ref, wo_ref, len_ref, o_ref, kv_ref, first_ref,
                 xbuf, wbuf, acc, kvf, qbuf, obuf, kshort, vshort, klong, vlong, lens, order,
                 x_sem, w_sem, short_sem, long_sem, first_sem, len_sem):
    me = lax.axis_index("model")
    steps, rows, depth = xbuf.shape
    slots = wbuf.shape[0]
    heads, dim = qbuf.shape[1:]
    width = heads * dim
    context = klong.shape[1]
    unit = context // SHORT
    head_cols = pl.ds(pl.multiple_of(me * dim, dim), dim)

    def x_copy(s):
        cols = pl.ds(pl.multiple_of(s * depth, depth), depth)
        return pltpu.make_async_copy(x_ref.at[:, cols], xbuf.at[s], x_sem.at[s])

    def w_copies(s, slot):
        lines = pl.ds(pl.multiple_of(s * depth, depth), depth)
        return (
            pltpu.make_async_copy(wq_ref.at[lines], wbuf.at[slot, :, pl.ds(0, width)], w_sem.at[slot, 0]),
            pltpu.make_async_copy(wk_ref.at[lines, head_cols], wbuf.at[slot, :, pl.ds(width, dim)], w_sem.at[slot, 1]),
            pltpu.make_async_copy(wv_ref.at[lines, head_cols], wbuf.at[slot, :, pl.ds(width + dim, dim)], w_sem.at[slot, 2]),
        )

    def short_copies():
        lines = pl.ds(0, SHORT)
        return (pltpu.make_async_copy(kc_ref.at[:, me, lines], kshort, short_sem.at[0]),
                pltpu.make_async_copy(vc_ref.at[:, me, lines], vshort, short_sem.at[1]))

    def long_copies(b, slot):
        return (pltpu.make_async_copy(kc_ref.at[b, me], klong.at[slot], long_sem.at[0]),
                pltpu.make_async_copy(vc_ref.at[b, me], vlong.at[slot], long_sem.at[1]))

    len_copy = pltpu.make_async_copy(len_ref, lens, len_sem)
    for s in range(slots):
        x_copy(s).start()
        for copy in w_copies(s, s):
            copy.start()
        if s == 0:
            len_copy.start()

    @pl.loop(slots, steps)
    def _(s):
        x_copy(s).start()

    def slab(j):
        cols = slab_cols(size, j, OFFSETS[0], first_ref.shape[2] // CORES)
        return pltpu.make_async_copy(wo_ref.at[:, cols], first_ref.at[j], first_sem.at[j])

    acc[...] = jnp.zeros_like(acc)
    len_copy.wait()

    def note(i, count):
        for j in range(unit):
            b = i * unit + j
            is_long = lens[b] > SHORT - 1

            @pl.when(is_long)
            def _():
                order[count] = b

            count = count + is_long.astype(jnp.int32)
        return count

    count = lax.fori_loop(0, rows // unit, note, jnp.int32(0))

    @pl.loop(0, steps)
    def _(s):
        slot = lax.rem(s, slots)
        x_copy(s).wait()
        for copy in w_copies(s, slot):
            copy.wait()
        acc[...] += jnp.dot(xbuf[s], wbuf[slot], preferred_element_type=F32)

        @pl.when(s + slots < steps)
        def _():
            for copy in w_copies(s + slots, slot):
                copy.start()

        @pl.when(s == steps - 2)
        def _():
            for copy in short_copies():
                copy.start()

            @pl.loop(0, count)
            def _(i):
                for copy in long_copies(order[i], i):
                    copy.start()

            for j in range(first_ref.shape[0]):
                slab(j).start()

    kv = acc[:, width:].astype(BF16)
    kv_ref[...] = kv
    kvf[...] = kv.astype(F32)
    for h in range(heads):
        qbuf[:, h, :] = acc[:, h * dim:(h + 1) * dim]

    inv_sqrt = dim ** -0.5
    contract_last = (((1,), (1,)), ((), ()))

    def iota(shape, axis):
        return lax.broadcasted_iota(jnp.int32, shape, axis)

    is_last = iota((PACK, dim), 0) == PACK - 1

    def put_new(keys, values, slot, size, b):
        lines = pl.ds(size - PACK, PACK)
        row = kvf[pl.ds(b, 1), :]
        new_key = jnp.broadcast_to(row[:, :dim], (PACK, dim)).astype(BF16)
        new_value = jnp.broadcast_to(row[:, dim:], (PACK, dim)).astype(BF16)
        keys[slot, lines, :] = jnp.where(is_last, new_key, keys[slot, lines, :])
        values[slot, lines, :] = jnp.where(is_last, new_value, values[slot, lines, :])

    def attend(items):
        scores = [lax.dot_general(q, keys, contract_last, preferred_element_type=F32) for q, keys, _, _ in items]
        weights, norms = [], []
        for score, (_, _, _, valid) in zip(scores, items):
            score = jnp.where(valid, score * inv_sqrt, -jnp.inf)
            weight = jnp.exp(score - jnp.max(score, axis=-1, keepdims=True))
            norms.append(jnp.sum(weight, axis=-1, keepdims=True))
            weights.append(weight.astype(BF16))
        totals = [jnp.dot(weight, item[2], preferred_element_type=F32) for weight, item in zip(weights, items)]
        return [total / norm for total, norm in zip(totals, norms)]

    for copy in short_copies():
        copy.wait()

    @pl.loop(0, rows // unit)
    def _(u):
        for j in range(unit):
            put_new(kshort, vshort, u * unit + j, SHORT, u * unit + j)

    short_rows = unit * heads
    col = iota((short_rows, context), 1)
    own = col // SHORT == iota((short_rows, 1), 0) // heads
    place = jnp.where(own, jnp.where(col % SHORT == SHORT - 1, -1, col % SHORT), context)
    line = iota((1, context), 1)

    @pl.loop(0, rows // unit // SHORT_STEP)
    def _(group):
        items, places = [], []
        for i in range(SHORT_STEP):
            first = (group * SHORT_STEP + i) * unit
            bound = jnp.zeros((1, context), jnp.int32)
            for j in range(unit):
                bound = jnp.where(line // SHORT == j, lens[first + j], bound)
            seqs = pl.ds(pl.multiple_of(first, unit), unit)
            places.append(seqs)
            items.append((
                qbuf[seqs].reshape(short_rows, dim).astype(BF16),
                kshort[seqs].reshape(context, dim), vshort[seqs].reshape(context, dim), place < bound))
        for seqs, out in zip(places, attend(items)):
            obuf[seqs] = out.reshape(unit, heads, dim)

    @pl.loop(0, count)
    def _(i):
        for copy in long_copies(0, 0):
            copy.wait()

    @pl.loop(0, count)
    def _(i):
        put_new(klong, vlong, i, context, order[i])

    long_col = iota((heads, context), 1)
    long_place = jnp.where(long_col == context - 1, -1, long_col)

    @pl.loop(0, (count + LONG_STEP - 1) // LONG_STEP)
    def _(i):
        slots = [jnp.minimum(i * LONG_STEP + j, count - 1) for j in range(LONG_STEP)]
        seqs = [order[slot] for slot in slots]
        outs = attend([(qbuf[b].astype(BF16), klong[slot], vlong[slot], long_place < lens[b])
                       for slot, b in zip(slots, seqs)])
        for b, out in zip(seqs, outs):
            obuf[b] = out

    for h in range(heads):
        o_ref[:, h * dim:(h + 1) * dim] = obuf[:, h, :].astype(BF16)
    for j in range(first_ref.shape[0]):
        slab(j).wait()


def front(size, x, w_query, w_key, w_value, k_cache, v_cache, w_out, lengths):
    rows, model = x.shape
    width = w_query.shape[1]
    context, dim = k_cache.shape[2:]
    heads = width // dim
    steps = model // DEPTH
    sem = pltpu.SemaphoreType.DMA
    total = width + 2 * dim
    first = pltpu.VMEM((len(OFFSETS), width, model // (ROUNDS * size) * CORES), BF16)
    return pl.pallas_call(
        functools.partial(front_kernel, size),
        out_shape=(pltpu.VMEM((rows, width), BF16), pltpu.VMEM((rows, 2 * dim), BF16), first),
        in_specs=[pl.BlockSpec(memory_space=pl.ANY)] * 7 + [pl.BlockSpec(memory_space=pltpu.HBM)],
        out_specs=(pl.BlockSpec(memory_space=pltpu.VMEM),) * 3,
        scratch_shapes=[
            pltpu.VMEM((steps, rows, DEPTH), BF16),
            pltpu.VMEM((4, DEPTH, total), BF16),
            pltpu.VMEM((rows, total), F32),
            pltpu.VMEM((rows, 2 * dim), F32),
            pltpu.VMEM((rows, heads, dim), F32),
            pltpu.VMEM((rows, heads, dim), F32),
            pltpu.VMEM((rows, SHORT, dim), BF16),
            pltpu.VMEM((rows, SHORT, dim), BF16),
            pltpu.VMEM((rows, context, dim), BF16),
            pltpu.VMEM((rows, context, dim), BF16),
            pltpu.SMEM((rows,), jnp.int32),
            pltpu.SMEM((rows,), jnp.int32),
            sem((steps,)), sem((4, 3)), sem((2,)), sem((2,)), sem((len(OFFSETS),)), sem,
        ],
        compiler_params=pltpu.CompilerParams(vmem_limit_bytes=48 * 1024 * 1024),
        cost_estimate=pl.CostEstimate(
            flops=2 * rows * model * total, bytes_accessed=model * total * 2, transcendentals=0),
        name="front",
    )(x, w_query, w_key, w_value, k_cache, v_cache, w_out, lengths)


def slab_cols(size, r, offset, n):
    chips = size // CORES
    dest = lax.rem(lax.axis_index("model") // CORES + offset, chips)
    return pl.ds(pl.multiple_of((r * chips + dest) * (CORES * n), CORES * n), CORES * n)


def out_kernel(size, o_ref, kv_ref, first_ref, x_ref, w_ref, y_ref, k_ref, v_ref,
               kvs_ref, kv_heads, wbuf, xbuf, part, pair, hop, near,
               w_sem, x_sem, kv_sem, pair_send, pair_recv, hop_send, hop_recv, near_send, near_recv,
               ag_send, ag_recv, fwd_send, fwd_recv):
    me = lax.axis_index("model")
    core = lax.rem(me, CORES)
    plus = lax.rem(me + CORES, size)
    minus = lax.rem(me + size - CORES, size)
    mate = me + 1 - 2 * core
    plus2 = lax.rem(me + 2 * CORES, size)
    rows, depth = o_ref.shape
    half = rows // 2
    slots = wbuf.shape[0]
    n, nk = part.shape[-1], kv_ref.shape[1]
    width = n * size
    top, bottom = pl.ds(0, half), pl.ds(half, half)
    kv_round = ROUNDS

    def slab(r, offset, slot):
        return pltpu.make_async_copy(w_ref.at[:, slab_cols(size, r, offset, n)], wbuf.at[slot], w_sem.at[slot])

    def own_x(r):
        cols = pl.ds(pl.multiple_of(r * width + me * n, n), n)
        return pltpu.make_async_copy(x_ref.at[:, cols], xbuf.at[r], x_sem.at[r])

    def remote(src, dst, send, recv, to):
        return pltpu.make_async_remote_copy(
            src_ref=src, dst_ref=dst, send_sem=send, recv_sem=recv,
            device_id={"model": to}, device_id_type=MESH)

    def pair_copy(r, j):
        return remote(part.at[r, j, 1 - core], pair.at[r, j], pair_send.at[r, j], pair_recv.at[r, j], mate)

    def hop_copy(r, way):
        to, lines = ((plus, top), (minus, bottom))[way]
        return remote(part.at[r, 0, core, lines], hop.at[r, way], hop_send.at[r, way], hop_recv.at[r, way], to)

    def near_copy(r, way):
        return remote(part.at[r, 1 + way, core], near.at[r, way], near_send.at[r, way], near_recv.at[r, way],
                      (plus, minus)[way])

    def block(r, owner, lines):
        if r is None:
            return kvs_ref.at[lines, pl.ds(pl.multiple_of(owner * nk, nk), nk)]
        return y_ref.at[lines, pl.ds(pl.multiple_of(r * width + owner * n, n), n)]

    everything = pl.ds(0, rows)

    def gather_copy(r, k):
        i = kv_round if r is None else r
        ref = block(r, me, everything)
        return remote(ref, ref, ag_send.at[i, k], ag_recv.at[i, k], (mate, plus, minus)[k])

    def relay_copy(r, way):
        i = kv_round if r is None else r
        ref = block(r, (minus, plus)[way], (top, bottom)[way])
        return remote(ref, ref, ag_send.at[i, 3 + way], ag_recv.at[i, 3 + way], (plus, minus)[way])

    def relayed_recv(r, way):
        i = kv_round if r is None else r
        ref = block(r, plus2, (top, bottom)[way])
        return remote(ref, ref, ag_send.at[i, 3 + way], ag_recv.at[i, 3 + way], (plus, minus)[way])

    def received(r, k):
        i = kv_round if r is None else r
        ref = block(r, (mate, minus, plus)[k], everything)
        return remote(ref, ref, ag_send.at[i, k], ag_recv.at[i, k], (mate, plus, minus)[k])

    def fwd_copy(r, k):
        i = kv_round if r is None else r
        owner, lines = ((minus, everything), (plus, everything), (plus2, top), (plus2, bottom))[k]
        ref = block(r, owner, lines)
        return remote(ref, ref, fwd_send.at[i, k], fwd_recv.at[i, k], mate)

    def fwd_recv_copy(r, k):
        i = kv_round if r is None else r
        flip = 1 - 2 * core
        owner, lines = ((minus, everything), (plus, everything), (plus2, top), (plus2, bottom))[k]
        ref = block(r, owner + flip, lines)
        return remote(ref, ref, fwd_send.at[i, k], fwd_recv.at[i, k], mate)

    for slot in range(slots):
        slab(slots + slot, OFFSETS[0], slot).start()
    own_kv = pltpu.make_async_copy(kv_ref, kvs_ref.at[:, pl.ds(pl.multiple_of(me * nk, nk), nk)], kv_sem)
    own_kv.start()

    barrier = pltpu.get_barrier_semaphore()
    for to in (mate, plus, minus):
        pl.semaphore_signal(barrier, inc=1, device_id={"model": to}, device_id_type=MESH)

    @pl.loop(0, ROUNDS)
    def _(r):
        own_x(r).start()

    own_kv.wait()
    pl.semaphore_wait(barrier, 3)
    for k in range(3):
        gather_copy(None, k).start()

    def pair_sum(r, j):
        pair_copy(r, j).wait_recv()
        part[r, j, core] = part[r, j, core] + pair[r, j]

    def send_hops(r):
        pair_sum(r, 0)
        for way in range(2):
            hop_copy(r, way).start()

    def send_near(r, way):
        pair_sum(r, 1 + way)
        hop_copy(r, way).wait_recv()
        lines = (top, bottom)[way]
        part[r, 1 + way, core, lines] = part[r, 1 + way, core, lines] + hop[r, way]
        near_copy(r, way).start()

    def relay(r):
        for way in range(2):
            received(r, 1 + way).wait_recv()
            relay_copy(r, way).start()
            fwd_copy(r, way).start()

    def pass_far(r):
        for way in range(2):
            relayed_recv(r, way).wait_recv()
            fwd_copy(r, 2 + way).start()

    def multiply(r, j, weights):
        product = jnp.dot(o_ref[...], weights[...], preferred_element_type=F32)
        for q in range(CORES):
            part[r, j, q] = product[:, q * n:(q + 1) * n]
        pair_copy(r, j).start()

    @pl.loop(0, slots)
    def _(r):
        multiply(r, 0, first_ref.at[r])

        @pl.when(r >= 2)
        def _():
            send_hops(r - 2)

    @pl.loop(slots, ROUNDS)
    def _(r):
        slot = r - slots
        slab(r, OFFSETS[0], slot).wait()
        multiply(r, 0, wbuf.at[slot])
        slab(slot // 2, OFFSETS[1] + 2 * lax.rem(slot, 2), slot).start()
        send_hops(r - 2)

    relay(None)

    @pl.loop(0, ROUNDS)
    def _(r):
        for way in range(2):
            slot = 2 * lax.rem(r, 2) + way
            slab(r, OFFSETS[1 + way], slot).wait()
            multiply(r, 1 + way, wbuf.at[slot])

            @pl.when(r < ROUNDS - 2)
            def _():
                slab(r + 2, OFFSETS[1 + way], slot).start()

            @pl.when(r >= ROUNDS - 2)
            def _():
                slab(2 * (r - (ROUNDS - 2)) + way, OFFSETS[3], slot).start()

            @pl.when(r == 0)
            def _():
                send_hops(ROUNDS - 2 + way)

            @pl.when(r >= 1)
            def _():
                send_near(r - 1, way)

    pass_far(None)

    @pl.loop(0, ROUNDS)
    def _(r):
        slot = lax.rem(r, slots)
        slab(r, OFFSETS[3], slot).wait()
        multiply(r, 3, wbuf.at[slot])

        @pl.when(r < ROUNDS - slots)
        def _():
            slab(r + slots, OFFSETS[3], slot).start()

        for way in range(2):
            @pl.when(r == way)
            def _():
                send_near(ROUNDS - 1, way)

        @pl.when(r >= 2)
        def _():
            pair_sum(r - 2, 3)

    for r in (ROUNDS - 2, ROUNDS - 1):
        pair_sum(r, 3)

    def drain(r):
        received(r, 0).wait_recv()
        for k in range(4):
            fwd_recv_copy(r, k).wait_recv()
        for k in range(3):
            gather_copy(r, k).wait_send()
        for way in range(2):
            relay_copy(r, way).wait_send()
        for k in range(4):
            fwd_copy(r, k).wait_send()

    drain(None)
    dim = nk // 2
    for i, ref in enumerate((k_ref, v_ref)):
        for owner in range(size):
            kv_heads[:, owner, :] = kvs_ref[:, owner * nk + i * dim:owner * nk + (i + 1) * dim].astype(F32)
        ref[...] = kv_heads[...].astype(BF16)

    def finish(r):
        for way in range(2):
            near_copy(r, way).wait_recv()
        own_x(r).wait()
        total = part[r, 3, core] + (near[r, 0] + near[r, 1])
        total = xbuf[r].astype(F32) + total
        y_ref[:, pl.ds(pl.multiple_of(r * width + me * n, n), n)] = total.astype(BF16)
        for k in range(3):
            gather_copy(r, k).start()

    @pl.loop(0, ROUNDS)
    def _(r):
        finish(r)

    @pl.loop(0, ROUNDS)
    def _(r):
        relay(r)

    @pl.loop(0, ROUNDS)
    def _(r):
        pass_far(r)

    @pl.loop(0, ROUNDS)
    def _(r):
        for j in range(4):
            pair_copy(r, j).wait_send()
        for way in range(2):
            hop_copy(r, way).wait_send()
            near_copy(r, way).wait_send()
        drain(r)


def out_product(size, o, kv, first, x, w_out):
    rows, depth = o.shape
    model = w_out.shape[1]
    n = model // (ROUNDS * size)
    sem = pltpu.SemaphoreType.DMA
    return pl.pallas_call(
        functools.partial(out_kernel, size),
        out_shape=(pltpu.VMEM((rows, model), BF16),) + (pltpu.VMEM((rows, size, kv.shape[1] // 2), BF16),) * 2,
        in_specs=[
            pl.BlockSpec(memory_space=pltpu.VMEM),
            pl.BlockSpec(memory_space=pl.ANY),
            pl.BlockSpec(memory_space=pltpu.VMEM),
            pl.BlockSpec(memory_space=pl.ANY),
            pl.BlockSpec(memory_space=pl.ANY),
        ],
        out_specs=(pl.BlockSpec(memory_space=pltpu.VMEM),) * 3,
        scratch_shapes=[
            pltpu.VMEM((rows, size * kv.shape[1]), BF16),
            pltpu.VMEM((rows, size, kv.shape[1] // 2), F32),
            pltpu.VMEM((4, depth, CORES * n), BF16),
            pltpu.VMEM((ROUNDS, rows, n), BF16),
            pltpu.VMEM((ROUNDS, 4, CORES, rows, n), F32),
            pltpu.VMEM((ROUNDS, 4, rows, n), F32),
            pltpu.VMEM((ROUNDS, 2, rows // 2, n), F32),
            pltpu.VMEM((ROUNDS, 2, rows, n), F32),
            sem((4,)), sem((ROUNDS,)), sem,
            sem((ROUNDS, 4)), sem((ROUNDS, 4)),
            sem((ROUNDS, 2)), sem((ROUNDS, 2)),
            sem((ROUNDS, 2)), sem((ROUNDS, 2)),
            sem((ROUNDS + 1, 5)), sem((ROUNDS + 1, 5)),
            sem((ROUNDS + 1, 4)), sem((ROUNDS + 1, 4)),
        ],
        compiler_params=pltpu.CompilerParams(
            collective_id=0, has_side_effects=True, vmem_limit_bytes=36 * 1024 * 1024),
        cost_estimate=pl.CostEstimate(
            flops=2 * rows * depth * model, bytes_accessed=depth * model * 2, transcendentals=0),
        name="out_reduce",
    )(o, kv, first, x, w_out)


def write_kernel(y_ref, k_ref, v_ref, y_out, k_out, v_out, sem):
    lines = y_ref.shape[0] // WRITES
    copies = [pltpu.make_async_copy(y_ref.at[pl.ds(i * lines, lines)], y_out.at[pl.ds(i * lines, lines)], sem.at[i])
              for i in range(WRITES)]
    copies.append(pltpu.make_async_copy(k_ref, k_out, sem.at[WRITES]))
    copies.append(pltpu.make_async_copy(v_ref, v_out, sem.at[WRITES + 1]))
    for copy in copies:
        copy.start()
    for copy in copies:
        copy.wait()


def write(*arrays):
    return pl.pallas_call(
        write_kernel,
        out_shape=tuple(jax.ShapeDtypeStruct(a.shape, a.dtype) for a in arrays),
        in_specs=[pl.BlockSpec(memory_space=pltpu.VMEM)] * 3,
        out_specs=(pl.BlockSpec(memory_space=pltpu.HBM),) * 3,
        scratch_shapes=[pltpu.SemaphoreType.DMA((WRITES + 2,))],
        compiler_params=pltpu.CompilerParams(vmem_limit_bytes=1024 * 1024),
        name="write",
    )(*arrays)


def solution(mesh):
    size = mesh.shape["model"]

    def local_step(x, w_query, w_key, w_value, w_out, k_cache, v_cache, lengths):
        x = pltpu.with_memory_space_constraint(x, pltpu.HBM)
        lengths = pltpu.with_memory_space_constraint(lengths, pltpu.HBM)
        out, kv, first = front(size, x, w_query, w_key, w_value, k_cache, v_cache, w_out, lengths)
        return write(*out_product(size, out, kv, first, x, w_out))

    rows_spec = P("replica")
    return jax.shard_map(
        local_step,
        mesh=mesh,
        in_specs=(P("replica", None), P(None, "model"), P(), P(), P("model", None), rows_spec, rows_spec, rows_spec),
        out_specs=(rows_spec, rows_spec, rows_spec),
        check_vma=False,
    )
```

```python
import functools

import jax
import jax.numpy as jnp
from jax import lax
from jax.experimental import pallas as pl
from jax.experimental.pallas import tpu as pltpu
from jax.sharding import PartitionSpec as P

MESH = pl.DeviceIdType.MESH
CORES = 2
ROUNDS = 8
WRITES = 8
DEPTH = 512
SHORT = 32
SHORT_STEP = 4
PACK = 16
LONG_STEP = 10
OFFSETS = (2, 1, 3, 0)
BF16 = jnp.bfloat16
F32 = jnp.float32


def front_kernel(size, x_ref, wq_ref, wk_ref, wv_ref, kc_ref, vc_ref, wo_ref, len_ref, o_ref, kv_ref, first_ref,
                 xbuf, wbuf, acc, kvf, qbuf, obuf, kshort, vshort, klong, vlong, lens, order,
                 x_sem, w_sem, short_sem, long_sem, first_sem, len_sem):
    me = lax.axis_index("model")
    steps, rows, depth = xbuf.shape
    slots = wbuf.shape[0]
    dim = qbuf.shape[1]
    heads = qbuf.shape[0] // rows
    width = heads * dim
    context = klong.shape[1]
    unit = context // SHORT
    head_cols = pl.ds(pl.multiple_of(me * dim, dim), dim)

    def x_copy(s):
        cols = pl.ds(pl.multiple_of(s * depth, depth), depth)
        return pltpu.make_async_copy(x_ref.at[:, cols], xbuf.at[s], x_sem.at[lax.rem(s, slots)])

    def w_copies(s, slot):
        lines = pl.ds(pl.multiple_of(s * depth, depth), depth)
        return [pltpu.make_async_copy(src, wbuf.at[slot, :, pl.ds(at, size)], w_sem.at[slot]) for src, at, size in (
            (wq_ref.at[lines], 0, width), (wk_ref.at[lines, head_cols], width, dim),
            (wv_ref.at[lines, head_cols], width + dim, dim))]

    def short_copies():
        lines = pl.ds(0, SHORT)
        return (pltpu.make_async_copy(kc_ref.at[:, me, lines], kshort, short_sem.at[0]),
                pltpu.make_async_copy(vc_ref.at[:, me, lines], vshort, short_sem.at[1]))

    def long_copies(b, slot):
        return (pltpu.make_async_copy(kc_ref.at[b, me], klong.at[slot], long_sem.at[0]),
                pltpu.make_async_copy(vc_ref.at[b, me], vlong.at[slot], long_sem.at[1]))

    len_copy = pltpu.make_async_copy(len_ref, lens, len_sem)
    for s in range(slots):
        x_copy(s).start()
        for copy in w_copies(s, s):
            copy.start()
        if s == 0:
            len_copy.start()

    def slab(j):
        cols = slab_cols(size, j, OFFSETS[0], first_ref.shape[2] // CORES)
        return pltpu.make_async_copy(wo_ref.at[:, cols], first_ref.at[j], first_sem)

    acc[...] = jnp.zeros_like(acc)
    len_copy.wait()

    def note(i, count):
        for j in range(unit):
            b = i * unit + j
            is_long = lens[b] > SHORT - 1

            @pl.when(is_long)
            def _():
                order[count] = b

            count = count + is_long.astype(jnp.int32)
        return count

    count = lax.fori_loop(0, rows // unit, note, jnp.int32(0))

    @pl.loop(0, steps)
    def _(s):
        slot = lax.rem(s, slots)
        x_copy(s).wait()
        pltpu.make_async_copy(wbuf.at[slot], wbuf.at[slot], w_sem.at[slot]).wait()
        acc[...] += jnp.dot(xbuf[s], wbuf[slot], preferred_element_type=F32)

        @pl.when(s + slots < steps)
        def _():
            x_copy(s + slots).start()
            for copy in w_copies(s + slots, slot):
                copy.start()

        @pl.when(s == steps - 2)
        def _():
            for copy in short_copies():
                copy.start()

            @pl.loop(0, count)
            def _(i):
                for copy in long_copies(order[i], i):
                    copy.start()

            for j in range(first_ref.shape[0]):
                slab(j).start()

    kv = acc[:, width:].astype(BF16)
    kv_ref[...] = kv
    kvf[...] = kv.astype(F32)
    for h in range(heads):
        qbuf[pl.ds(h, rows, stride=heads), :] = acc[:, h * dim:(h + 1) * dim]

    inv_sqrt = dim ** -0.5
    contract_last = (((1,), (1,)), ((), ()))

    def iota(shape, axis):
        return lax.broadcasted_iota(jnp.int32, shape, axis)

    is_last = iota((PACK, dim), 0) == PACK - 1

    def put_new(keys, values, slot, size, b):
        lines = pl.ds(size - PACK, PACK)
        row = kvf[pl.ds(b, 1), :]
        new_key = jnp.broadcast_to(row[:, :dim], (PACK, dim)).astype(BF16)
        new_value = jnp.broadcast_to(row[:, dim:], (PACK, dim)).astype(BF16)
        keys[slot, lines, :] = jnp.where(is_last, new_key, keys[slot, lines, :])
        values[slot, lines, :] = jnp.where(is_last, new_value, values[slot, lines, :])

    def attend(items):
        scores = [lax.dot_general(q, keys, contract_last, preferred_element_type=F32) for q, keys, _, _ in items]
        weights, norms = [], []
        for score, (_, _, _, valid) in zip(scores, items):
            score = jnp.where(valid, score * inv_sqrt, -jnp.inf)
            weight = jnp.exp(score - jnp.max(score, axis=-1, keepdims=True))
            norms.append(jnp.sum(weight, axis=-1, keepdims=True))
            weights.append(weight.astype(BF16))
        totals = [jnp.dot(weight, item[2], preferred_element_type=F32) for weight, item in zip(weights, items)]
        return [total / norm for total, norm in zip(totals, norms)]

    for copy in short_copies():
        copy.wait()

    @pl.loop(0, rows // unit)
    def _(u):
        for j in range(unit):
            put_new(kshort, vshort, u * unit + j, SHORT, u * unit + j)

    short_rows = unit * heads
    col = iota((short_rows, context), 1)
    own = col // SHORT == iota((short_rows, 1), 0) // heads
    place = jnp.where(own, jnp.where(col % SHORT == SHORT - 1, -1, col % SHORT), context)
    line = iota((1, context), 1)

    @pl.loop(0, rows // unit // SHORT_STEP)
    def _(group):
        items, places = [], []
        for i in range(SHORT_STEP):
            first = (group * SHORT_STEP + i) * unit
            bound = jnp.zeros((1, context), jnp.int32)
            for j in range(unit):
                bound = jnp.where(line // SHORT == j, lens[first + j], bound)
            seqs = pl.ds(pl.multiple_of(first, unit), unit)
            lines = pl.ds(pl.multiple_of(first * heads, short_rows), short_rows)
            places.append(lines)
            items.append((
                qbuf[lines].astype(BF16),
                kshort[seqs].reshape(context, dim), vshort[seqs].reshape(context, dim), place < bound))
        for lines, out in zip(places, attend(items)):
            obuf[lines] = out

    @pl.loop(0, count)
    def _(i):
        for copy in long_copies(0, 0):
            copy.wait()

    @pl.loop(0, count)
    def _(i):
        put_new(klong, vlong, i, context, order[i])

    long_col = iota((heads, context), 1)
    long_place = jnp.where(long_col == context - 1, -1, long_col)

    @pl.loop(0, (count + LONG_STEP - 1) // LONG_STEP)
    def _(i):
        slots = [jnp.minimum(i * LONG_STEP + j, count - 1) for j in range(LONG_STEP)]
        seqs = [order[slot] for slot in slots]
        lines = [pl.ds(pl.multiple_of(b * heads, heads), heads) for b in seqs]
        outs = attend([(qbuf[here].astype(BF16), klong[slot], vlong[slot], long_place < lens[b])
                       for here, slot, b in zip(lines, slots, seqs)])
        for here, out in zip(lines, outs):
            obuf[here] = out

    for h in range(heads):
        o_ref[:, h * dim:(h + 1) * dim] = obuf[pl.ds(h, rows, stride=heads), :].astype(BF16)
    pltpu.make_async_copy(first_ref, first_ref, first_sem).wait()


def front(size, x, w_query, w_key, w_value, k_cache, v_cache, w_out, lengths):
    rows, model = x.shape
    width = w_query.shape[1]
    context, dim = k_cache.shape[2:]
    heads = width // dim
    steps = model // DEPTH
    sem = pltpu.SemaphoreType.DMA
    total = width + 2 * dim
    first = pltpu.VMEM((len(OFFSETS), width, model // (ROUNDS * size) * CORES), BF16)
    return pl.pallas_call(
        functools.partial(front_kernel, size),
        out_shape=(pltpu.VMEM((rows, width), BF16), pltpu.VMEM((rows, 2 * dim), BF16), first),
        in_specs=[pl.BlockSpec(memory_space=pl.ANY)] * 7 + [pl.BlockSpec(memory_space=pltpu.HBM)],
        out_specs=(pl.BlockSpec(memory_space=pltpu.VMEM),) * 3,
        scratch_shapes=[
            pltpu.VMEM((steps, rows, DEPTH), BF16),
            pltpu.VMEM((4, DEPTH, total), BF16),
            pltpu.VMEM((rows, total), F32),
            pltpu.VMEM((rows, 2 * dim), F32),
            pltpu.VMEM((rows * heads, dim), F32),
            pltpu.VMEM((rows * heads, dim), F32),
            pltpu.VMEM((rows, SHORT, dim), BF16),
            pltpu.VMEM((rows, SHORT, dim), BF16),
            pltpu.VMEM((rows, context, dim), BF16),
            pltpu.VMEM((rows, context, dim), BF16),
            pltpu.SMEM((rows,), jnp.int32),
            pltpu.SMEM((rows,), jnp.int32),
            sem((4,)), sem((4,)), sem((2,)), sem((2,)), sem, sem,
        ],
        compiler_params=pltpu.CompilerParams(vmem_limit_bytes=48 * 1024 * 1024),
        cost_estimate=pl.CostEstimate(
            flops=2 * rows * model * total, bytes_accessed=model * total * 2, transcendentals=0),
        name="front",
    )(x, w_query, w_key, w_value, k_cache, v_cache, w_out, lengths)


def slab_cols(size, r, offset, n):
    chips = size // CORES
    dest = lax.rem(lax.axis_index("model") // CORES + offset, chips)
    return pl.ds(pl.multiple_of((r * chips + dest) * (CORES * n), CORES * n), CORES * n)


def out_kernel(size, o_ref, kv_ref, first_ref, x_ref, w_ref, y_ref, k_ref, v_ref,
               kvs_ref, kv_heads, wbuf, xbuf, part, pair, hop, near,
               w_sem, x_sem, kv_sem, sent, pair_recv, hop_recv, near_recv, ag_recv, relay_recv, mate_recv):
    me = lax.axis_index("model")
    core = lax.rem(me, CORES)
    plus = lax.rem(me + CORES, size)
    minus = lax.rem(me + size - CORES, size)
    mate = me + 1 - 2 * core
    plus2 = lax.rem(me + 2 * CORES, size)
    rows, depth = o_ref.shape
    half = rows // 2
    slots = wbuf.shape[0]
    n, nk = part.shape[-1], kv_ref.shape[1]
    width = n * size
    top, bottom = pl.ds(0, half), pl.ds(half, half)
    kv_round = ROUNDS

    def slab(r, offset, slot):
        return pltpu.make_async_copy(w_ref.at[:, slab_cols(size, r, offset, n)], wbuf.at[slot], w_sem.at[slot])

    def own_x(r):
        cols = pl.ds(pl.multiple_of(r * width + me * n, n), n)
        return pltpu.make_async_copy(x_ref.at[:, cols], xbuf.at[r], x_sem)

    def remote(src, dst, send, recv, to):
        return pltpu.make_async_remote_copy(
            src_ref=src, dst_ref=dst, send_sem=send, recv_sem=recv,
            device_id={"model": to}, device_id_type=MESH)

    PAIR, HOP, NEAR, GATHER, FORWARD = range(5)

    def pair_copy(r, j):
        recv = pair_recv.at[(len(OFFSETS) - 1) * ROUNDS if j == len(OFFSETS) - 1 else j * ROUNDS + r]
        return remote(part.at[r, j, 1 - core], pair.at[r, j], sent.at[PAIR], recv, mate)

    def hop_copy(r, way):
        to, lines = ((plus, top), (minus, bottom))[way]
        return remote(part.at[r, 0, core, lines], hop.at[r, way], sent.at[HOP], hop_recv.at[r], to)

    def near_copy(r, way):
        return remote(part.at[r, 1 + way, core], near.at[r, way], sent.at[NEAR], near_recv.at[r], (plus, minus)[way])

    def block(r, owner, lines):
        if r is None:
            return kvs_ref.at[lines, pl.ds(pl.multiple_of(owner * nk, nk), nk)]
        return y_ref.at[lines, pl.ds(pl.multiple_of(r * width + owner * n, n), n)]

    def blocks(r, count):
        if r is None:
            return kvs_ref.at[:, pl.ds(0, count * nk)]
        return y_ref.at[:, pl.ds(0, count * n)]

    everything = pl.ds(0, rows)

    def sems(r):
        i, kind = (ROUNDS, 1) if r is None else (r, 0)
        return sent.at[GATHER + 2 * kind], sent.at[FORWARD + 2 * kind], ag_recv.at[i], relay_recv.at[i], mate_recv.at[kind]

    def wait_for(ref, sem):
        remote(ref, ref, sem, sem, mate).wait_recv()

    def gather(r):
        send, _, recv, _, mate_sem = sems(r)
        ref = block(r, me, everything)
        for to, sem in ((plus, recv), (minus, recv), (mate, mate_sem)):
            remote(ref, ref, send, sem, to).start()

    def forward(r, owner, lines):
        _, send, _, _, sem = sems(r)
        ref = block(r, owner, lines)
        remote(ref, ref, send, sem, mate).start()

    def relay(r):
        send, _, recv, relay_sem, _ = sems(r)
        wait_for(blocks(r, 2), recv)
        for owner, lines, to in ((minus, top, plus), (plus, bottom, minus)):
            ref = block(r, owner, lines)
            remote(ref, ref, send, relay_sem, to).start()
        for owner in (minus, plus):
            forward(r, owner, everything)

    def pass_far(r):
        _, _, _, sem, _ = sems(r)
        wait_for(blocks(r, 1), sem)
        forward(r, plus2, everything)

    for slot in range(slots):
        slab(slots + slot, OFFSETS[0], slot).start()
    own_kv = pltpu.make_async_copy(kv_ref, kvs_ref.at[:, pl.ds(pl.multiple_of(me * nk, nk), nk)], kv_sem)
    own_kv.start()

    barrier = pltpu.get_barrier_semaphore()
    for to in (mate, plus, minus):
        pl.semaphore_signal(barrier, inc=1, device_id={"model": to}, device_id_type=MESH)

    @pl.loop(0, ROUNDS)
    def _(r):
        own_x(r).start()

    own_kv.wait()
    pl.semaphore_wait(barrier, 3)
    gather(None)

    def pair_sum(r, j):
        pair_copy(r, j).wait_recv()
        part[r, j, core] = part[r, j, core] + pair[r, j]

    def send_hops(r):
        pair_sum(r, 0)
        for way in range(2):
            hop_copy(r, way).start()

    def send_near(r, way):
        pair_sum(r, 1 + way)
        if way == 0:
            wait_for(hop.at[r], hop_recv.at[r])
        lines = (top, bottom)[way]
        part[r, 1 + way, core, lines] = part[r, 1 + way, core, lines] + hop[r, way]
        near_copy(r, way).start()

    def multiply(r, j, weights):
        product = jnp.dot(o_ref[...], weights[...], preferred_element_type=F32)
        for q in range(CORES):
            part[r, j, q] = product[:, q * n:(q + 1) * n]
        pair_copy(r, j).start()

    @pl.loop(0, slots)
    def _(r):
        multiply(r, 0, first_ref.at[r])

        @pl.when(r >= 2)
        def _():
            send_hops(r - 2)

    @pl.loop(slots, ROUNDS)
    def _(r):
        slot = r - slots
        slab(r, OFFSETS[0], slot).wait()
        multiply(r, 0, wbuf.at[slot])
        slab(slot // 2, OFFSETS[1] + 2 * lax.rem(slot, 2), slot).start()
        send_hops(r - 2)

    relay(None)

    @pl.loop(0, ROUNDS)
    def _(r):
        for way in range(2):
            slot = 2 * lax.rem(r, 2) + way
            slab(r, OFFSETS[1 + way], slot).wait()
            multiply(r, 1 + way, wbuf.at[slot])

            @pl.when(r < ROUNDS - 2)
            def _():
                slab(r + 2, OFFSETS[1 + way], slot).start()

            @pl.when(r >= ROUNDS - 2)
            def _():
                slab(2 * (r - (ROUNDS - 2)) + way, OFFSETS[3], slot).start()

            @pl.when(r == 0)
            def _():
                send_hops(ROUNDS - 2 + way)

            @pl.when(r >= 1)
            def _():
                send_near(r - 1, way)

    pass_far(None)

    @pl.loop(0, ROUNDS)
    def _(r):
        slot = lax.rem(r, slots)
        slab(r, OFFSETS[3], slot).wait()
        multiply(r, 3, wbuf.at[slot])

        @pl.when(r < ROUNDS - slots)
        def _():
            slab(r + slots, OFFSETS[3], slot).start()

        for way in range(2):
            @pl.when(r == way)
            def _():
                send_near(ROUNDS - 1, way)

    wait_for(blocks(None, 4), mate_recv.at[1])
    dim = nk // 2
    for i, ref in enumerate((k_ref, v_ref)):
        for owner in range(size):
            kv_heads[pl.ds(owner, rows, stride=size), :] = kvs_ref[:, owner * nk + i * dim:owner * nk + (i + 1) * dim].astype(F32)
        ref[...] = kv_heads[...].astype(BF16).reshape(ref.shape)

    wait_for(pair.at[:, 3], pair_recv.at[3 * ROUNDS])
    pltpu.make_async_copy(xbuf, xbuf, x_sem).wait()

    @pl.loop(0, ROUNDS)
    def _(r):
        wait_for(near.at[r], near_recv.at[r])
        total = (part[r, 3, core] + pair[r, 3]) + (near[r, 0] + near[r, 1])
        total = xbuf[r].astype(F32) + total
        y_ref[:, pl.ds(pl.multiple_of(r * width + me * n, n), n)] = total.astype(BF16)
        gather(r)

    @pl.loop(0, ROUNDS)
    def _(r):
        relay(r)

    @pl.loop(0, ROUNDS)
    def _(r):
        pass_far(r)

    wait_for(blocks(0, 4 * ROUNDS), mate_recv.at[0])
    for ref, kind in ((pair, PAIR), (hop, HOP), (near, NEAR), (blocks(0, 4 * ROUNDS), GATHER), (blocks(0, 3 * ROUNDS), FORWARD),
                      (blocks(None, 4), GATHER + 2), (blocks(None, 3), FORWARD + 2)):
        wait_for(ref, sent.at[kind])


def out_product(size, o, kv, first, x, w_out):
    rows, depth = o.shape
    model = w_out.shape[1]
    n = model // (ROUNDS * size)
    sem = pltpu.SemaphoreType.DMA
    return pl.pallas_call(
        functools.partial(out_kernel, size),
        out_shape=(pltpu.VMEM((rows, model), BF16),) + (pltpu.VMEM((rows, size, kv.shape[1] // 2), BF16),) * 2,
        in_specs=[
            pl.BlockSpec(memory_space=pltpu.VMEM),
            pl.BlockSpec(memory_space=pl.ANY),
            pl.BlockSpec(memory_space=pltpu.VMEM),
            pl.BlockSpec(memory_space=pl.ANY),
            pl.BlockSpec(memory_space=pl.ANY),
        ],
        out_specs=(pl.BlockSpec(memory_space=pltpu.VMEM),) * 3,
        scratch_shapes=[
            pltpu.VMEM((rows, size * kv.shape[1]), BF16),
            pltpu.VMEM((rows * size, kv.shape[1] // 2), F32),
            pltpu.VMEM((4, depth, CORES * n), BF16),
            pltpu.VMEM((ROUNDS, rows, n), BF16),
            pltpu.VMEM((ROUNDS, 4, CORES, rows, n), F32),
            pltpu.VMEM((ROUNDS, 4, rows, n), F32),
            pltpu.VMEM((ROUNDS, 2, rows // 2, n), F32),
            pltpu.VMEM((ROUNDS, 2, rows, n), F32),
            sem((4,)), sem, sem, sem((7,)),
            sem((3 * ROUNDS + 1,)), sem((ROUNDS,)), sem((ROUNDS,)), sem((ROUNDS + 1,)), sem((ROUNDS + 1,)), sem((2,)),
        ],
        compiler_params=pltpu.CompilerParams(
            collective_id=0, has_side_effects=True, vmem_limit_bytes=36 * 1024 * 1024),
        cost_estimate=pl.CostEstimate(
            flops=2 * rows * depth * model, bytes_accessed=depth * model * 2, transcendentals=0),
        name="out_reduce",
    )(o, kv, first, x, w_out)


def write_kernel(y_ref, k_ref, v_ref, y_out, k_out, v_out, sem):
    lines = y_ref.shape[0] // WRITES
    copies = [pltpu.make_async_copy(y_ref.at[pl.ds(i * lines, lines)], y_out.at[pl.ds(i * lines, lines)], sem.at[i])
              for i in range(WRITES)]
    copies.append(pltpu.make_async_copy(k_ref, k_out, sem.at[WRITES]))
    copies.append(pltpu.make_async_copy(v_ref, v_out, sem.at[WRITES + 1]))
    for copy in copies:
        copy.start()
    for copy in copies:
        copy.wait()


def write(*arrays):
    return pl.pallas_call(
        write_kernel,
        out_shape=tuple(jax.ShapeDtypeStruct(a.shape, a.dtype) for a in arrays),
        in_specs=[pl.BlockSpec(memory_space=pltpu.VMEM)] * 3,
        out_specs=(pl.BlockSpec(memory_space=pltpu.HBM),) * 3,
        scratch_shapes=[pltpu.SemaphoreType.DMA((WRITES + 2,))],
        compiler_params=pltpu.CompilerParams(vmem_limit_bytes=1024 * 1024),
        name="write",
    )(*arrays)


def solution(mesh):
    size = mesh.shape["model"]

    def local_step(x, w_query, w_key, w_value, w_out, k_cache, v_cache, lengths):
        x = pltpu.with_memory_space_constraint(x, pltpu.HBM)
        lengths = pltpu.with_memory_space_constraint(lengths, pltpu.HBM)
        out, kv, first = front(size, x, w_query, w_key, w_value, k_cache, v_cache, w_out, lengths)
        return write(*out_product(size, out, kv, first, x, w_out))

    rows_spec = P("replica")
    return jax.shard_map(
        local_step,
        mesh=mesh,
        in_specs=(P("replica", None), P(None, "model"), P(), P(), P("model", None), rows_spec, rows_spec, rows_spec),
        out_specs=(rows_spec, rows_spec, rows_spec),
        check_vma=False,
    )
```

```python
import functools

import jax
import jax.numpy as jnp
from jax import lax
from jax.experimental import pallas as pl
from jax.experimental.pallas import tpu as pltpu
from jax.sharding import PartitionSpec as P

MESH = pl.DeviceIdType.MESH
CORES = 2
ROUNDS = 8
FIRST = 2
WRITES = 8
DEPTH = 1024
SHORT = 32
SHORT_STEP = 8
PITCH = 24
PACK = 16
LONG_STEP = 10
OFFSETS = (2, 1, 3, 0)
BF16 = jnp.bfloat16
F32 = jnp.float32


def front_kernel(size, x_ref, wq_ref, wk_ref, wv_ref, kc_ref, vc_ref, wo_ref, len_ref, o_ref, kv_ref, first_ref,
                 xbuf, wbuf, acc, kvf, qbuf, obuf, kshort, vshort, klong, vlong, lens, order,
                 x_sem, w_sem, short_sem, long_sem, first_sem, len_sem):
    me = lax.axis_index("model")
    steps, rows, depth = xbuf.shape
    slots = wbuf.shape[0]
    dim = qbuf.shape[2]
    heads = o_ref.shape[1] // dim
    qflat, oflat = (ref.reshape(rows * PITCH, dim) for ref in (qbuf, obuf))
    lines = pl.ds(0, heads)
    width = heads * dim
    context = klong.shape[1]
    unit = context // SHORT
    head_cols = pl.ds(pl.multiple_of(me * dim, dim), dim)

    def x_copy(s):
        cols = pl.ds(pl.multiple_of(s * depth, depth), depth)
        return pltpu.make_async_copy(x_ref.at[:, cols], xbuf.at[s], x_sem.at[lax.rem(s, slots)])

    def w_copies(s, slot):
        lines = pl.ds(pl.multiple_of(s * depth, depth), depth)
        return [pltpu.make_async_copy(src, wbuf.at[slot, :, pl.ds(at, size)], w_sem.at[slot]) for src, at, size in (
            (wq_ref.at[lines], 0, width), (wk_ref.at[lines, head_cols], width, dim),
            (wv_ref.at[lines, head_cols], width + dim, dim))]

    def short_copies():
        lines = pl.ds(0, SHORT)
        return (pltpu.make_async_copy(kc_ref.at[:, me, lines], kshort, short_sem.at[0]),
                pltpu.make_async_copy(vc_ref.at[:, me, lines], vshort, short_sem.at[1]))

    def long_copies(b, slot):
        return (pltpu.make_async_copy(kc_ref.at[b, me], klong.at[slot], long_sem.at[0]),
                pltpu.make_async_copy(vc_ref.at[b, me], vlong.at[slot], long_sem.at[1]))

    len_copy = pltpu.make_async_copy(len_ref, lens, len_sem)
    for s in range(slots):
        x_copy(s).start()
        for copy in w_copies(s, s):
            copy.start()
        if s == 0:
            len_copy.start()

    def slab(j):
        cols = slab_cols(size, j, OFFSETS[0], first_ref.shape[2] // CORES)
        return pltpu.make_async_copy(wo_ref.at[:, cols], first_ref.at[j], first_sem)

    acc[...] = jnp.zeros_like(acc)
    len_copy.wait()

    def note(i, count):
        for j in range(unit):
            b = i * unit + j
            is_long = lens[b] > SHORT - 1

            @pl.when(is_long)
            def _():
                order[count] = b

            count = count + is_long.astype(jnp.int32)
        return count

    count = lax.fori_loop(0, rows // unit, note, jnp.int32(0))

    @pl.loop(0, steps)
    def _(s):
        slot = lax.rem(s, slots)
        x_copy(s).wait()
        pltpu.make_async_copy(wbuf.at[slot], wbuf.at[slot], w_sem.at[slot]).wait()
        acc[...] += jnp.dot(xbuf[s], wbuf[slot], preferred_element_type=F32)

        @pl.when(s + slots < steps)
        def _():
            x_copy(s + slots).start()
            for copy in w_copies(s + slots, slot):
                copy.start()

        @pl.when(s == steps - 2)
        def _():
            for copy in short_copies():
                copy.start()

            @pl.loop(0, count)
            def _(i):
                for copy in long_copies(order[i], i):
                    copy.start()

            for j in range(first_ref.shape[0]):
                slab(j).start()

    kv = acc[:, width:].astype(BF16)
    kv_ref[...] = kv
    kvf[...] = kv.astype(F32)
    for h in range(heads):
        qflat[pl.ds(h, rows, stride=PITCH), :] = acc[:, h * dim:(h + 1) * dim]

    inv_sqrt = dim ** -0.5
    contract_last = (((1,), (1,)), ((), ()))

    def iota(shape, axis):
        return lax.broadcasted_iota(jnp.int32, shape, axis)

    is_last = iota((PACK, dim), 0) == PACK - 1

    def put_new(keys, values, slot, size, b):
        lines = pl.ds(size - PACK, PACK)
        row = kvf[pl.ds(b, 1), :]
        new_key = jnp.broadcast_to(row[:, :dim], (PACK, dim)).astype(BF16)
        new_value = jnp.broadcast_to(row[:, dim:], (PACK, dim)).astype(BF16)
        keys[slot, lines, :] = jnp.where(is_last, new_key, keys[slot, lines, :])
        values[slot, lines, :] = jnp.where(is_last, new_value, values[slot, lines, :])

    def attend(items):
        scores = [lax.dot_general(q, keys, contract_last, preferred_element_type=F32) for q, keys, _, _ in items]
        weights, norms = [], []
        for score, (_, _, _, valid) in zip(scores, items):
            score = jnp.where(valid, score * inv_sqrt, -jnp.inf)
            weight = jnp.exp(score - jnp.max(score, axis=-1, keepdims=True))
            norms.append(jnp.sum(weight, axis=-1, keepdims=True))
            weights.append(weight.astype(BF16))
        totals = [jnp.dot(weight, item[2], preferred_element_type=F32) for weight, item in zip(weights, items)]
        return [total / norm for total, norm in zip(totals, norms)]

    for copy in short_copies():
        copy.wait()

    @pl.loop(0, rows // unit)
    def _(u):
        for j in range(unit):
            put_new(kshort, vshort, u * unit + j, SHORT, u * unit + j)

    short_rows = unit * heads
    col = iota((short_rows, context), 1)
    own = col // SHORT == iota((short_rows, 1), 0) // heads
    place = jnp.where(own, jnp.where(col % SHORT == SHORT - 1, -1, col % SHORT), context)
    line = iota((1, context), 1)

    def short_items(group):
        items = []
        for i in range(SHORT_STEP):
            first = (group * SHORT_STEP + i) * unit
            bound = jnp.zeros((1, context), jnp.int32)
            for j in range(unit):
                bound = jnp.where(line // SHORT == j, lens[first + j], bound)
            seqs = pl.ds(pl.multiple_of(first, unit), unit)
            items.append((
                seqs, qbuf[seqs, lines].reshape(short_rows, dim).astype(BF16),
                kshort[seqs].reshape(context, dim), vshort[seqs].reshape(context, dim), place < bound))
        return items

    long_col = iota((heads, context), 1)
    long_place = jnp.where(long_col == context - 1, -1, long_col)

    def long_items(i):
        items = []
        for j in range(LONG_STEP):
            slot = jnp.minimum(i * LONG_STEP + j, count - 1)
            b = order[slot]
            items.append((b, qbuf[b, lines].astype(BF16), klong[slot], vlong[slot], long_place < lens[b]))
        return items

    def work(items):
        for item, out in zip(items, attend([item[1:] for item in items])):
            here = obuf.at[item[0], lines]
            here[...] = out.reshape(here.shape)

    @pl.loop(0, count)
    def _(i):
        for copy in long_copies(0, 0):
            copy.wait()

    @pl.loop(0, count)
    def _(i):
        put_new(klong, vlong, i, context, order[i])

    last = rows // unit // SHORT_STEP - 1

    @pl.loop(0, last)
    def _(group):
        work(short_items(group))

    work(short_items(last) + long_items(0))

    @pl.loop(1, (count + LONG_STEP - 1) // LONG_STEP)
    def _(i):
        work(long_items(i))

    for h in range(heads):
        o_ref[:, h * dim:(h + 1) * dim] = oflat[pl.ds(h, rows, stride=PITCH), :].astype(BF16)
    pltpu.make_async_copy(first_ref, first_ref, first_sem).wait()


def front(size, x, w_query, w_key, w_value, k_cache, v_cache, w_out, lengths):
    rows, model = x.shape
    width = w_query.shape[1]
    context, dim = k_cache.shape[2:]
    heads = width // dim
    steps = model // DEPTH
    sem = pltpu.SemaphoreType.DMA
    total = width + 2 * dim
    first = pltpu.VMEM((FIRST, width, model // (ROUNDS * size) * CORES), BF16)
    return pl.pallas_call(
        functools.partial(front_kernel, size),
        out_shape=(pltpu.VMEM((rows, width), BF16), pltpu.VMEM((rows, 2 * dim), BF16), first),
        in_specs=[pl.BlockSpec(memory_space=pl.ANY)] * 7 + [pl.BlockSpec(memory_space=pltpu.HBM)],
        out_specs=(pl.BlockSpec(memory_space=pltpu.VMEM),) * 3,
        scratch_shapes=[
            pltpu.VMEM((steps, rows, DEPTH), BF16),
            pltpu.VMEM((3, DEPTH, total), BF16),
            pltpu.VMEM((rows, total), F32),
            pltpu.VMEM((rows, 2 * dim), F32),
            pltpu.VMEM((rows, PITCH, dim), F32),
            pltpu.VMEM((rows, PITCH, dim), F32),
            pltpu.VMEM((rows, SHORT, dim), BF16),
            pltpu.VMEM((rows, SHORT, dim), BF16),
            pltpu.VMEM((rows, context, dim), BF16),
            pltpu.VMEM((rows, context, dim), BF16),
            pltpu.SMEM((rows,), jnp.int32),
            pltpu.SMEM((rows,), jnp.int32),
            sem((3,)), sem((3,)), sem((2,)), sem((2,)), sem, sem,
        ],
        compiler_params=pltpu.CompilerParams(vmem_limit_bytes=48 * 1024 * 1024),
        cost_estimate=pl.CostEstimate(
            flops=2 * rows * model * total, bytes_accessed=model * total * 2, transcendentals=0),
        name="front",
    )(x, w_query, w_key, w_value, k_cache, v_cache, w_out, lengths)


def slab_cols(size, r, offset, n):
    chips = size // CORES
    dest = lax.rem(lax.axis_index("model") // CORES + offset, chips)
    return pl.ds(pl.multiple_of((r * chips + dest) * (CORES * n), CORES * n), CORES * n)


def out_kernel(size, o_ref, kv_ref, first_ref, x_ref, w_ref, y_ref, k_ref, v_ref,
               kvs_ref, kv_heads, wbuf, xbuf, part, pair, hop, near,
               w_sem, x_sem, kv_sem, sent, pair_recv, hop_recv, near_recv, ag_recv, relay_recv, mate_recv):
    me = lax.axis_index("model")
    core = lax.rem(me, CORES)
    plus = lax.rem(me + CORES, size)
    minus = lax.rem(me + size - CORES, size)
    mate = me + 1 - 2 * core
    plus2 = lax.rem(me + 2 * CORES, size)
    rows, depth = o_ref.shape
    half = rows // 2
    slots = wbuf.shape[0]
    n, nk = part.shape[-1], kv_ref.shape[1]
    width = n * size
    top, bottom = pl.ds(0, half), pl.ds(half, half)
    kv_round = ROUNDS

    def slab(r, offset, slot):
        return pltpu.make_async_copy(w_ref.at[:, slab_cols(size, r, offset, n)], wbuf.at[slot], w_sem.at[slot])

    def own_x(r):
        cols = pl.ds(pl.multiple_of(r * width + me * n, n), n)
        return pltpu.make_async_copy(x_ref.at[:, cols], xbuf.at[r], x_sem)

    def remote(src, dst, send, recv, to):
        return pltpu.make_async_remote_copy(
            src_ref=src, dst_ref=dst, send_sem=send, recv_sem=recv,
            device_id={"model": to}, device_id_type=MESH)

    PAIR, HOP, NEAR, GATHER, FORWARD = range(5)

    def pair_copy(r, j):
        recv = pair_recv.at[(len(OFFSETS) - 1) * ROUNDS if j == len(OFFSETS) - 1 else j * ROUNDS + r]
        return remote(part.at[r, j, 1 - core], pair.at[r, j], sent.at[PAIR], recv, mate)

    def hop_copy(r, way):
        to, lines = ((plus, top), (minus, bottom))[way]
        return remote(part.at[r, 0, core, lines], hop.at[r, way], sent.at[HOP], hop_recv.at[r], to)

    def near_copy(r, way):
        return remote(part.at[r, 1 + way, core], near.at[r, way], sent.at[NEAR], near_recv.at[r], (plus, minus)[way])

    def block(r, owner, lines):
        if r is None:
            return kvs_ref.at[lines, pl.ds(pl.multiple_of(owner * nk, nk), nk)]
        return y_ref.at[lines, pl.ds(pl.multiple_of(r * width + owner * n, n), n)]

    def blocks(r, count):
        if r is None:
            return kvs_ref.at[:, pl.ds(0, count * nk)]
        return y_ref.at[:, pl.ds(0, count * n)]

    everything = pl.ds(0, rows)

    def sems(r):
        i, kind = (ROUNDS, 1) if r is None else (r, 0)
        return sent.at[GATHER + 2 * kind], sent.at[FORWARD + 2 * kind], ag_recv.at[i], relay_recv.at[i], mate_recv.at[kind]

    def wait_for(ref, sem):
        remote(ref, ref, sem, sem, mate).wait_recv()

    def gather(r):
        send, _, recv, _, mate_sem = sems(r)
        ref = block(r, me, everything)
        for to, sem in ((plus, recv), (minus, recv), (mate, mate_sem)):
            remote(ref, ref, send, sem, to).start()

    def forward(r, owner, lines):
        _, send, _, _, sem = sems(r)
        ref = block(r, owner, lines)
        remote(ref, ref, send, sem, mate).start()

    def relay(r):
        send, _, recv, relay_sem, _ = sems(r)
        wait_for(blocks(r, 2), recv)
        for owner, lines, to in ((minus, top, plus), (plus, bottom, minus)):
            ref = block(r, owner, lines)
            remote(ref, ref, send, relay_sem, to).start()
        for owner in (minus, plus):
            forward(r, owner, everything)

    def pass_far(r):
        _, _, _, sem, _ = sems(r)
        wait_for(blocks(r, 1), sem)
        forward(r, plus2, everything)

    for slot in range(slots):
        slab(FIRST + slot, OFFSETS[0], slot).start()
    own_kv = pltpu.make_async_copy(kv_ref, kvs_ref.at[:, pl.ds(pl.multiple_of(me * nk, nk), nk)], kv_sem)
    own_kv.start()

    barrier = pltpu.get_barrier_semaphore()
    for to in (mate, plus, minus):
        pl.semaphore_signal(barrier, inc=1, device_id={"model": to}, device_id_type=MESH)

    @pl.loop(0, ROUNDS)
    def _(r):
        own_x(r).start()

    own_kv.wait()
    pl.semaphore_wait(barrier, 3)
    gather(None)

    def pair_sum(r, j):
        pair_copy(r, j).wait_recv()
        part[r, j, core] = part[r, j, core] + pair[r, j]

    def send_hops(r):
        pair_sum(r, 0)
        for way in range(2):
            hop_copy(r, way).start()

    def send_near(r, way):
        pair_sum(r, 1 + way)
        if way == 0:
            wait_for(hop.at[r], hop_recv.at[r])
        lines = (top, bottom)[way]
        part[r, 1 + way, core, lines] = part[r, 1 + way, core, lines] + hop[r, way]
        near_copy(r, way).start()

    def multiply(r, j, weights):
        product = jnp.dot(o_ref[...], weights[...], preferred_element_type=F32)
        for q in range(CORES):
            part[r, j, q] = product[:, q * n:(q + 1) * n]
        pair_copy(r, j).start()

    @pl.loop(0, FIRST)
    def _(r):
        multiply(r, 0, first_ref.at[r])

    @pl.loop(FIRST, ROUNDS)
    def _(r):
        slot = lax.rem(r - FIRST, slots)
        slab(r, OFFSETS[0], slot).wait()
        multiply(r, 0, wbuf.at[slot])

        @pl.when(r < ROUNDS - slots)
        def _():
            slab(r + slots, OFFSETS[0], slot).start()

        @pl.when(r >= ROUNDS - slots)
        def _():
            ahead = r - (ROUNDS - slots)
            slab(ahead // 2, OFFSETS[1] + 2 * lax.rem(ahead, 2), slot).start()

        send_hops(r - 2)

    relay(None)

    @pl.loop(0, ROUNDS)
    def _(r):
        for way in range(2):
            slot = lax.rem(2 * r + way + ROUNDS - FIRST, slots)
            slab(r, OFFSETS[1 + way], slot).wait()
            multiply(r, 1 + way, wbuf.at[slot])

            @pl.when(r < ROUNDS - 2)
            def _():
                slab(r + 2, OFFSETS[1 + way], slot).start()

            @pl.when(r >= ROUNDS - 2)
            def _():
                slab(2 * (r - (ROUNDS - 2)) + way, OFFSETS[3], slot).start()

            @pl.when(r == 0)
            def _():
                send_hops(ROUNDS - 2 + way)

            @pl.when(r >= 1)
            def _():
                send_near(r - 1, way)

    pass_far(None)

    @pl.loop(0, ROUNDS)
    def _(r):
        slot = lax.rem(r + 3 * ROUNDS - FIRST, slots)
        slab(r, OFFSETS[3], slot).wait()
        multiply(r, 3, wbuf.at[slot])

        @pl.when(r < ROUNDS - slots)
        def _():
            slab(r + slots, OFFSETS[3], slot).start()

        for way in range(2):
            @pl.when(r == way)
            def _():
                send_near(ROUNDS - 1, way)

    wait_for(blocks(None, 4), mate_recv.at[1])
    dim = nk // 2
    for i, ref in enumerate((k_ref, v_ref)):
        for owner in range(size):
            kv_heads[pl.ds(owner, rows, stride=size), :] = kvs_ref[:, owner * nk + i * dim:owner * nk + (i + 1) * dim].astype(F32)
        ref[...] = kv_heads[...].astype(BF16).reshape(ref.shape)

    wait_for(pair.at[:, 3], pair_recv.at[3 * ROUNDS])
    pltpu.make_async_copy(xbuf, xbuf, x_sem).wait()

    @pl.loop(0, ROUNDS)
    def _(r):
        wait_for(near.at[r], near_recv.at[r])
        total = (part[r, 3, core] + pair[r, 3]) + (near[r, 0] + near[r, 1])
        total = xbuf[r].astype(F32) + total
        y_ref[:, pl.ds(pl.multiple_of(r * width + me * n, n), n)] = total.astype(BF16)
        gather(r)

    @pl.loop(0, ROUNDS)
    def _(r):
        relay(r)

    @pl.loop(0, ROUNDS)
    def _(r):
        pass_far(r)

    wait_for(blocks(0, 4 * ROUNDS), mate_recv.at[0])
    for ref, kind in ((pair, PAIR), (hop, HOP), (near, NEAR), (blocks(0, 4 * ROUNDS), GATHER), (blocks(0, 3 * ROUNDS), FORWARD),
                      (blocks(None, 4), GATHER + 2), (blocks(None, 3), FORWARD + 2)):
        wait_for(ref, sent.at[kind])


def out_product(size, o, kv, first, x, w_out):
    rows, depth = o.shape
    model = w_out.shape[1]
    n = model // (ROUNDS * size)
    sem = pltpu.SemaphoreType.DMA
    return pl.pallas_call(
        functools.partial(out_kernel, size),
        out_shape=(pltpu.VMEM((rows, model), BF16),) + (pltpu.VMEM((rows, size, kv.shape[1] // 2), BF16),) * 2,
        in_specs=[
            pl.BlockSpec(memory_space=pltpu.VMEM),
            pl.BlockSpec(memory_space=pl.ANY),
            pl.BlockSpec(memory_space=pltpu.VMEM),
            pl.BlockSpec(memory_space=pl.ANY),
            pl.BlockSpec(memory_space=pl.ANY),
        ],
        out_specs=(pl.BlockSpec(memory_space=pltpu.VMEM),) * 3,
        scratch_shapes=[
            pltpu.VMEM((rows, size * kv.shape[1]), BF16),
            pltpu.VMEM((rows * size, kv.shape[1] // 2), F32),
            pltpu.VMEM((4, depth, CORES * n), BF16),
            pltpu.VMEM((ROUNDS, rows, n), BF16),
            pltpu.VMEM((ROUNDS, 4, CORES, rows, n), F32),
            pltpu.VMEM((ROUNDS, 4, rows, n), F32),
            pltpu.VMEM((ROUNDS, 2, rows // 2, n), F32),
            pltpu.VMEM((ROUNDS, 2, rows, n), F32),
            sem((4,)), sem, sem, sem((7,)),
            sem((3 * ROUNDS + 1,)), sem((ROUNDS,)), sem((ROUNDS,)), sem((ROUNDS + 1,)), sem((ROUNDS + 1,)), sem((2,)),
        ],
        compiler_params=pltpu.CompilerParams(
            collective_id=0, has_side_effects=True, vmem_limit_bytes=36 * 1024 * 1024),
        cost_estimate=pl.CostEstimate(
            flops=2 * rows * depth * model, bytes_accessed=depth * model * 2, transcendentals=0),
        name="out_reduce",
    )(o, kv, first, x, w_out)


def write_kernel(y_ref, k_ref, v_ref, y_out, k_out, v_out, sem):
    lines = y_ref.shape[0] // WRITES
    copies = [pltpu.make_async_copy(y_ref.at[pl.ds(i * lines, lines)], y_out.at[pl.ds(i * lines, lines)], sem.at[i])
              for i in range(WRITES)]
    copies.append(pltpu.make_async_copy(k_ref, k_out, sem.at[WRITES]))
    copies.append(pltpu.make_async_copy(v_ref, v_out, sem.at[WRITES + 1]))
    for copy in copies:
        copy.start()
    for copy in copies:
        copy.wait()


def write(*arrays):
    return pl.pallas_call(
        write_kernel,
        out_shape=tuple(jax.ShapeDtypeStruct(a.shape, a.dtype) for a in arrays),
        in_specs=[pl.BlockSpec(memory_space=pltpu.VMEM)] * 3,
        out_specs=(pl.BlockSpec(memory_space=pltpu.HBM),) * 3,
        scratch_shapes=[pltpu.SemaphoreType.DMA((WRITES + 2,))],
        compiler_params=pltpu.CompilerParams(vmem_limit_bytes=1024 * 1024),
        name="write",
    )(*arrays)


def solution(mesh):
    size = mesh.shape["model"]

    def local_step(x, w_query, w_key, w_value, w_out, k_cache, v_cache, lengths):
        x = pltpu.with_memory_space_constraint(x, pltpu.HBM)
        lengths = pltpu.with_memory_space_constraint(lengths, pltpu.HBM)
        out, kv, first = front(size, x, w_query, w_key, w_value, k_cache, v_cache, w_out, lengths)
        return write(*out_product(size, out, kv, first, x, w_out))

    rows_spec = P("replica")
    return jax.shard_map(
        local_step,
        mesh=mesh,
        in_specs=(P("replica", None), P(None, "model"), P(), P(), P("model", None), rows_spec, rows_spec, rows_spec),
        out_specs=(rows_spec, rows_spec, rows_spec),
        check_vma=False,
    )
```

```python
import functools

import jax
import jax.numpy as jnp
from jax import lax
from jax.experimental import pallas as pl
from jax.experimental.pallas import tpu as pltpu
from jax.sharding import PartitionSpec as P

MESH = pl.DeviceIdType.MESH
CORES = 2
ROUNDS = 8
FIRST = 2
WRITES = 2
DEPTH = 1024
SHORT = 32
SHORT_STEP = 8
PITCH = 24
PACK = 16
LONG_STEP = 10
OFFSETS = (2, 1, 3, 0)
BF16 = jnp.bfloat16
F32 = jnp.float32


def front_kernel(size, x_ref, wq_ref, wk_ref, wv_ref, kc_ref, vc_ref, wo_ref, len_ref, o_ref, kv_ref, first_ref,
                 xbuf, wbuf, acc, kvf, qbuf, obuf, kshort, vshort, klong, vlong, lens, order,
                 x_sem, w_sem, short_sem, long_sem, first_sem, len_sem):
    me = lax.axis_index("model")
    steps, rows, depth = xbuf.shape
    slots = wbuf.shape[0]
    dim = qbuf.shape[2]
    heads = o_ref.shape[1] // dim
    qflat, oflat = (ref.reshape(rows * PITCH, dim) for ref in (qbuf, obuf))
    lines = pl.ds(0, heads)
    width = heads * dim
    context = klong.shape[1]
    unit = context // SHORT
    head_cols = pl.ds(pl.multiple_of(me * dim, dim), dim)

    def x_copy(s):
        cols = pl.ds(pl.multiple_of(s * depth, depth), depth)
        return pltpu.make_async_copy(x_ref.at[:, cols], xbuf.at[s], x_sem.at[lax.rem(s, slots)])

    def w_copies(s, slot):
        lines = pl.ds(pl.multiple_of(s * depth, depth), depth)
        return [pltpu.make_async_copy(src, wbuf.at[slot, :, pl.ds(at, size)], w_sem.at[slot]) for src, at, size in (
            (wq_ref.at[lines], 0, width), (wk_ref.at[lines, head_cols], width, dim),
            (wv_ref.at[lines, head_cols], width + dim, dim))]

    def short_copies():
        lines = pl.ds(0, SHORT)
        return (pltpu.make_async_copy(kc_ref.at[:, me, lines], kshort, short_sem.at[0]),
                pltpu.make_async_copy(vc_ref.at[:, me, lines], vshort, short_sem.at[1]))

    def long_copies(b, slot):
        return (pltpu.make_async_copy(kc_ref.at[b, me], klong.at[slot], long_sem.at[0]),
                pltpu.make_async_copy(vc_ref.at[b, me], vlong.at[slot], long_sem.at[1]))

    len_copy = pltpu.make_async_copy(len_ref, lens, len_sem)
    for s in range(slots):
        x_copy(s).start()
        for copy in w_copies(s, s):
            copy.start()
        if s == 0:
            len_copy.start()

    def slab(j):
        cols = slab_cols(size, j, OFFSETS[0], first_ref.shape[2] // CORES)
        return pltpu.make_async_copy(wo_ref.at[:, cols], first_ref.at[j], first_sem)

    acc[...] = jnp.zeros_like(acc)
    len_copy.wait()

    def note(i, count):
        for j in range(unit):
            b = i * unit + j
            is_long = lens[b] > SHORT - 1

            @pl.when(is_long)
            def _():
                order[count] = b

            count = count + is_long.astype(jnp.int32)
        return count

    count = lax.fori_loop(0, rows // unit, note, jnp.int32(0))

    @pl.loop(0, steps)
    def _(s):
        slot = lax.rem(s, slots)
        x_copy(s).wait()
        pltpu.make_async_copy(wbuf.at[slot], wbuf.at[slot], w_sem.at[slot]).wait()
        acc[...] += jnp.dot(xbuf[s], wbuf[slot], preferred_element_type=F32)

        @pl.when(s + slots < steps)
        def _():
            x_copy(s + slots).start()
            for copy in w_copies(s + slots, slot):
                copy.start()

        @pl.when(s == steps - 2)
        def _():
            for copy in short_copies():
                copy.start()

            @pl.loop(0, count)
            def _(i):
                for copy in long_copies(order[i], i):
                    copy.start()

            for j in range(first_ref.shape[0]):
                slab(j).start()

    kv = acc[:, width:].astype(BF16)
    kv_ref[...] = kv
    kvf[...] = kv.astype(F32)
    for h in range(heads):
        qflat[pl.ds(h, rows, stride=PITCH), :] = acc[:, h * dim:(h + 1) * dim]

    inv_sqrt = dim ** -0.5
    contract_last = (((1,), (1,)), ((), ()))

    def iota(shape, axis):
        return lax.broadcasted_iota(jnp.int32, shape, axis)

    is_last = iota((PACK, dim), 0) == PACK - 1

    def put_new(keys, values, slot, size, b):
        lines = pl.ds(size - PACK, PACK)
        row = kvf[pl.ds(b, 1), :]
        new_key = jnp.broadcast_to(row[:, :dim], (PACK, dim)).astype(BF16)
        new_value = jnp.broadcast_to(row[:, dim:], (PACK, dim)).astype(BF16)
        keys[slot, lines, :] = jnp.where(is_last, new_key, keys[slot, lines, :])
        values[slot, lines, :] = jnp.where(is_last, new_value, values[slot, lines, :])

    def attend(items):
        scores = [lax.dot_general(q, keys, contract_last, preferred_element_type=F32) for q, keys, _, _ in items]
        weights, norms = [], []
        for score, (_, _, _, valid) in zip(scores, items):
            score = jnp.where(valid, score * inv_sqrt, -jnp.inf)
            weight = jnp.exp(score - jnp.max(score, axis=-1, keepdims=True))
            norms.append(jnp.sum(weight, axis=-1, keepdims=True))
            weights.append(weight.astype(BF16))
        totals = [jnp.dot(weight, item[2], preferred_element_type=F32) for weight, item in zip(weights, items)]
        return [total / norm for total, norm in zip(totals, norms)]

    for copy in short_copies():
        copy.wait()

    short_rows = unit * heads
    col = iota((short_rows, context), 1)
    own = col // SHORT == iota((short_rows, 1), 0) // heads
    place = jnp.where(own, jnp.where(col % SHORT == SHORT - 1, -1, col % SHORT), context)
    line = iota((1, context), 1)

    def short_items(group):
        for i in range(SHORT_STEP * unit):
            put_new(kshort, vshort, group * SHORT_STEP * unit + i, SHORT, group * SHORT_STEP * unit + i)
        items = []
        for i in range(SHORT_STEP):
            first = (group * SHORT_STEP + i) * unit
            bound = jnp.zeros((1, context), jnp.int32)
            for j in range(unit):
                bound = jnp.where(line // SHORT == j, lens[first + j], bound)
            seqs = pl.ds(pl.multiple_of(first, unit), unit)
            items.append((
                seqs, qbuf[seqs, lines].reshape(short_rows, dim).astype(BF16),
                kshort[seqs].reshape(context, dim), vshort[seqs].reshape(context, dim), place < bound))
        return items

    long_col = iota((heads, context), 1)
    long_place = jnp.where(long_col == context - 1, -1, long_col)

    def long_items(i):
        items = []
        for j in range(LONG_STEP):
            slot = jnp.minimum(i * LONG_STEP + j, count - 1)
            b = order[slot]
            items.append((b, qbuf[b, lines].astype(BF16), klong[slot], vlong[slot], long_place < lens[b]))
        return items

    def work(items):
        for item, out in zip(items, attend([item[1:] for item in items])):
            here = obuf.at[item[0], lines]
            here[...] = out.reshape(here.shape)

    @pl.loop(0, count)
    def _(i):
        for copy in long_copies(0, 0):
            copy.wait()

    @pl.loop(0, count)
    def _(i):
        put_new(klong, vlong, i, context, order[i])

    last = rows // unit // SHORT_STEP - 1

    @pl.loop(0, last)
    def _(group):
        work(short_items(group))

    work(short_items(last) + long_items(0))

    @pl.loop(1, (count + LONG_STEP - 1) // LONG_STEP)
    def _(i):
        work(long_items(i))

    for h in range(heads):
        o_ref[:, h * dim:(h + 1) * dim] = oflat[pl.ds(h, rows, stride=PITCH), :].astype(BF16)
    pltpu.make_async_copy(first_ref, first_ref, first_sem).wait()


def front(size, x, w_query, w_key, w_value, k_cache, v_cache, w_out, lengths):
    rows, model = x.shape
    width = w_query.shape[1]
    context, dim = k_cache.shape[2:]
    heads = width // dim
    steps = model // DEPTH
    sem = pltpu.SemaphoreType.DMA
    total = width + 2 * dim
    first = pltpu.VMEM((FIRST, width, model // (ROUNDS * size) * CORES), BF16)
    return pl.pallas_call(
        functools.partial(front_kernel, size),
        out_shape=(pltpu.VMEM((rows, width), BF16), pltpu.VMEM((rows, 2 * dim), BF16), first),
        in_specs=[pl.BlockSpec(memory_space=pl.ANY)] * 7 + [pl.BlockSpec(memory_space=pltpu.HBM)],
        out_specs=(pl.BlockSpec(memory_space=pltpu.VMEM),) * 3,
        scratch_shapes=[
            pltpu.VMEM((steps, rows, DEPTH), BF16),
            pltpu.VMEM((3, DEPTH, total), BF16),
            pltpu.VMEM((rows, total), F32),
            pltpu.VMEM((rows, 2 * dim), F32),
            pltpu.VMEM((rows, PITCH, dim), F32),
            pltpu.VMEM((rows, PITCH, dim), F32),
            pltpu.VMEM((rows, SHORT, dim), BF16),
            pltpu.VMEM((rows, SHORT, dim), BF16),
            pltpu.VMEM((rows, context, dim), BF16),
            pltpu.VMEM((rows, context, dim), BF16),
            pltpu.SMEM((rows,), jnp.int32),
            pltpu.SMEM((rows,), jnp.int32),
            sem((3,)), sem((3,)), sem((2,)), sem((2,)), sem, sem,
        ],
        compiler_params=pltpu.CompilerParams(vmem_limit_bytes=48 * 1024 * 1024),
        cost_estimate=pl.CostEstimate(
            flops=2 * rows * model * total, bytes_accessed=model * total * 2, transcendentals=0),
        name="front",
    )(x, w_query, w_key, w_value, k_cache, v_cache, w_out, lengths)


def slab_cols(size, r, offset, n):
    chips = size // CORES
    dest = lax.rem(lax.axis_index("model") // CORES + offset, chips)
    return pl.ds(pl.multiple_of((r * chips + dest) * (CORES * n), CORES * n), CORES * n)


def out_kernel(size, o_ref, kv_ref, first_ref, x_ref, w_ref, y_ref, k_ref, v_ref,
               kvs_ref, kv_heads, wbuf, xbuf, part, pair, hop, near,
               w_sem, x_sem, kv_sem, sent, pair_recv, hop_recv, near_recv, ag_recv, relay_recv, mate_recv):
    me = lax.axis_index("model")
    core = lax.rem(me, CORES)
    plus = lax.rem(me + CORES, size)
    minus = lax.rem(me + size - CORES, size)
    mate = me + 1 - 2 * core
    plus2 = lax.rem(me + 2 * CORES, size)
    rows, depth = o_ref.shape
    half = rows // 2
    slots = wbuf.shape[0]
    n, nk = part.shape[-1], kv_ref.shape[1]
    width = n * size
    top, bottom = pl.ds(0, half), pl.ds(half, half)
    kv_round = ROUNDS

    def slab(r, offset, slot):
        return pltpu.make_async_copy(w_ref.at[:, slab_cols(size, r, offset, n)], wbuf.at[slot], w_sem.at[slot])

    def own_x(r):
        cols = pl.ds(pl.multiple_of(r * width + me * n, n), n)
        return pltpu.make_async_copy(x_ref.at[:, cols], xbuf.at[r], x_sem)

    def remote(src, dst, send, recv, to):
        return pltpu.make_async_remote_copy(
            src_ref=src, dst_ref=dst, send_sem=send, recv_sem=recv,
            device_id={"model": to}, device_id_type=MESH)

    PAIR, HOP, NEAR, GATHER, FORWARD = range(5)

    def pair_copy(r, j):
        recv = pair_recv.at[(0 * ROUNDS + r, ROUNDS + r, ROUNDS + r, 2 * ROUNDS)[j]]
        return remote(part.at[r, j, 1 - core], pair.at[r, j], sent.at[PAIR], recv, mate)

    def hop_copy(r, way):
        to, lines = ((plus, top), (minus, bottom))[way]
        return remote(part.at[r, 0, core, lines], hop.at[r, way], sent.at[HOP], hop_recv.at[r], to)

    def near_copy(r, way):
        return remote(part.at[r, 1 + way, core], near.at[r, way], sent.at[NEAR], near_recv.at[r], (plus, minus)[way])

    def block(r, owner, lines):
        if r is None:
            return kvs_ref.at[lines, pl.ds(pl.multiple_of(owner * nk, nk), nk)]
        return y_ref.at[lines, pl.ds(pl.multiple_of(r * width + owner * n, n), n)]

    def blocks(r, count):
        if r is None:
            return kvs_ref.at[:, pl.ds(0, count * nk)]
        return y_ref.at[:, pl.ds(0, count * n)]

    everything = pl.ds(0, rows)

    def sems(r):
        i, kind = (ROUNDS, 1) if r is None else (r, 0)
        return sent.at[GATHER + 2 * kind], sent.at[FORWARD + 2 * kind], ag_recv.at[i], relay_recv.at[i], mate_recv.at[kind]

    def wait_for(ref, sem):
        remote(ref, ref, sem, sem, mate).wait_recv()

    def gather(r):
        send, _, recv, _, mate_sem = sems(r)
        ref = block(r, me, everything)
        for to, sem in ((plus, recv), (minus, recv), (mate, mate_sem)):
            remote(ref, ref, send, sem, to).start()

    def forward(r, owner, lines):
        _, send, _, _, sem = sems(r)
        ref = block(r, owner, lines)
        remote(ref, ref, send, sem, mate).start()

    def relay(r):
        send, _, recv, relay_sem, _ = sems(r)
        wait_for(blocks(r, 2), recv)
        for owner, lines, to in ((minus, top, plus), (plus, bottom, minus)):
            ref = block(r, owner, lines)
            remote(ref, ref, send, relay_sem, to).start()
        for owner in (minus, plus):
            forward(r, owner, everything)

    def pass_far(r):
        _, _, _, sem, _ = sems(r)
        wait_for(blocks(r, 1), sem)
        forward(r, plus2, everything)

    for slot in range(slots):
        slab(FIRST + slot, OFFSETS[0], slot).start()
    own_kv = pltpu.make_async_copy(kv_ref, kvs_ref.at[:, pl.ds(pl.multiple_of(me * nk, nk), nk)], kv_sem)
    own_kv.start()

    barrier = pltpu.get_barrier_semaphore()
    for to in (mate, plus, minus):
        pl.semaphore_signal(barrier, inc=1, device_id={"model": to}, device_id_type=MESH)

    @pl.loop(0, ROUNDS)
    def _(r):
        own_x(r).start()

    own_kv.wait()
    pl.semaphore_wait(barrier, 3)
    gather(None)

    def pair_sum(r, j):
        if j == 0:
            pair_copy(r, j).wait_recv()
        elif j == 1:
            wait_for(pair.at[r, pl.ds(1, 2)], pair_recv.at[ROUNDS + r])
        part[r, j, core] = part[r, j, core] + pair[r, j]

    def send_hops(r):
        pair_sum(r, 0)
        for way in range(2):
            hop_copy(r, way).start()

    def send_near(r, way):
        pair_sum(r, 1 + way)
        if way == 0:
            wait_for(hop.at[r], hop_recv.at[r])
        lines = (top, bottom)[way]
        part[r, 1 + way, core, lines] = part[r, 1 + way, core, lines] + hop[r, way]
        near_copy(r, way).start()

    def multiply(r, j, weights):
        product = jnp.dot(o_ref[...], weights[...], preferred_element_type=F32)
        for q in range(CORES):
            part[r, j, q] = product[:, q * n:(q + 1) * n]
        pair_copy(r, j).start()

    @pl.loop(0, FIRST)
    def _(r):
        multiply(r, 0, first_ref.at[r])

    @pl.loop(FIRST, ROUNDS)
    def _(r):
        slot = lax.rem(r - FIRST, slots)
        slab(r, OFFSETS[0], slot).wait()
        multiply(r, 0, wbuf.at[slot])

        @pl.when(r < ROUNDS - slots)
        def _():
            slab(r + slots, OFFSETS[0], slot).start()

        @pl.when(r >= ROUNDS - slots)
        def _():
            ahead = r - (ROUNDS - slots)
            slab(ahead // 2, OFFSETS[1] + 2 * lax.rem(ahead, 2), slot).start()

        send_hops(r - 2)

    relay(None)

    @pl.loop(0, ROUNDS)
    def _(r):
        for way in range(2):
            slot = lax.rem(2 * r + way + ROUNDS - FIRST, slots)
            slab(r, OFFSETS[1 + way], slot).wait()
            multiply(r, 1 + way, wbuf.at[slot])

            @pl.when(r < ROUNDS - 2)
            def _():
                slab(r + 2, OFFSETS[1 + way], slot).start()

            @pl.when(r >= ROUNDS - 2)
            def _():
                slab(2 * (r - (ROUNDS - 2)) + way, OFFSETS[3], slot).start()

            @pl.when(r == 0)
            def _():
                send_hops(ROUNDS - 2 + way)

            @pl.when(r >= 1)
            def _():
                send_near(r - 1, way)

    pass_far(None)

    @pl.loop(0, ROUNDS)
    def _(r):
        slot = lax.rem(r + 3 * ROUNDS - FIRST, slots)
        slab(r, OFFSETS[3], slot).wait()
        multiply(r, 3, wbuf.at[slot])

        @pl.when(r < ROUNDS - slots)
        def _():
            slab(r + slots, OFFSETS[3], slot).start()

        for way in range(2):
            @pl.when(r == way)
            def _():
                send_near(ROUNDS - 1, way)

    wait_for(blocks(None, 4), mate_recv.at[1])
    dim = nk // 2
    for i, ref in enumerate((k_ref, v_ref)):
        for owner in range(size):
            kv_heads[pl.ds(owner, rows, stride=size), :] = kvs_ref[:, owner * nk + i * dim:owner * nk + (i + 1) * dim].astype(F32)
        ref[...] = kv_heads[...].astype(BF16).reshape(ref.shape)

    wait_for(pair.at[:, 3], pair_recv.at[2 * ROUNDS])
    pltpu.make_async_copy(xbuf, xbuf, x_sem).wait()

    @pl.loop(0, ROUNDS)
    def _(r):
        wait_for(near.at[r], near_recv.at[r])
        total = (part[r, 3, core] + pair[r, 3]) + (near[r, 0] + near[r, 1])
        total = xbuf[r].astype(F32) + total
        y_ref[:, pl.ds(pl.multiple_of(r * width + me * n, n), n)] = total.astype(BF16)
        gather(r)

    @pl.loop(0, ROUNDS)
    def _(r):
        relay(r)

    @pl.loop(0, ROUNDS)
    def _(r):
        pass_far(r)

    wait_for(blocks(0, 4 * ROUNDS), mate_recv.at[0])
    for ref, kind in ((pair, PAIR), (hop, HOP), (near, NEAR), (blocks(0, 4 * ROUNDS), GATHER), (blocks(0, 3 * ROUNDS), FORWARD),
                      (blocks(None, 4), GATHER + 2), (blocks(None, 3), FORWARD + 2)):
        wait_for(ref, sent.at[kind])


def out_product(size, o, kv, first, x, w_out):
    rows, depth = o.shape
    model = w_out.shape[1]
    n = model // (ROUNDS * size)
    sem = pltpu.SemaphoreType.DMA
    return pl.pallas_call(
        functools.partial(out_kernel, size),
        out_shape=(pltpu.VMEM((rows, model), BF16),) + (pltpu.VMEM((rows, size, kv.shape[1] // 2), BF16),) * 2,
        in_specs=[
            pl.BlockSpec(memory_space=pltpu.VMEM),
            pl.BlockSpec(memory_space=pl.ANY),
            pl.BlockSpec(memory_space=pltpu.VMEM),
            pl.BlockSpec(memory_space=pl.ANY),
            pl.BlockSpec(memory_space=pl.ANY),
        ],
        out_specs=(pl.BlockSpec(memory_space=pltpu.VMEM),) * 3,
        scratch_shapes=[
            pltpu.VMEM((rows, size * kv.shape[1]), BF16),
            pltpu.VMEM((rows * size, kv.shape[1] // 2), F32),
            pltpu.VMEM((4, depth, CORES * n), BF16),
            pltpu.VMEM((ROUNDS, rows, n), BF16),
            pltpu.VMEM((ROUNDS, 4, CORES, rows, n), F32),
            pltpu.VMEM((ROUNDS, 4, rows, n), F32),
            pltpu.VMEM((ROUNDS, 2, rows // 2, n), F32),
            pltpu.VMEM((ROUNDS, 2, rows, n), F32),
            sem((4,)), sem, sem, sem((7,)),
            sem((2 * ROUNDS + 1,)), sem((ROUNDS,)), sem((ROUNDS,)), sem((ROUNDS + 1,)), sem((ROUNDS + 1,)), sem((2,)),
        ],
        compiler_params=pltpu.CompilerParams(
            collective_id=0, has_side_effects=True, vmem_limit_bytes=36 * 1024 * 1024),
        cost_estimate=pl.CostEstimate(
            flops=2 * rows * depth * model, bytes_accessed=depth * model * 2, transcendentals=0),
        name="out_reduce",
    )(o, kv, first, x, w_out)


def write_kernel(y_ref, k_ref, v_ref, y_out, k_out, v_out, sem):
    lines = y_ref.shape[0] // WRITES
    copies = [pltpu.make_async_copy(y_ref.at[pl.ds(i * lines, lines)], y_out.at[pl.ds(i * lines, lines)], sem.at[i])
              for i in range(WRITES)]
    copies.append(pltpu.make_async_copy(k_ref, k_out, sem.at[WRITES]))
    copies.append(pltpu.make_async_copy(v_ref, v_out, sem.at[WRITES + 1]))
    for copy in copies:
        copy.start()
    for copy in copies:
        copy.wait()


def write(*arrays):
    return pl.pallas_call(
        write_kernel,
        out_shape=tuple(jax.ShapeDtypeStruct(a.shape, a.dtype) for a in arrays),
        in_specs=[pl.BlockSpec(memory_space=pltpu.VMEM)] * 3,
        out_specs=(pl.BlockSpec(memory_space=pltpu.HBM),) * 3,
        scratch_shapes=[pltpu.SemaphoreType.DMA((WRITES + 2,))],
        compiler_params=pltpu.CompilerParams(vmem_limit_bytes=1024 * 1024),
        name="write",
    )(*arrays)


def solution(mesh):
    size = mesh.shape["model"]

    def local_step(x, w_query, w_key, w_value, w_out, k_cache, v_cache, lengths):
        x = pltpu.with_memory_space_constraint(x, pltpu.HBM)
        lengths = pltpu.with_memory_space_constraint(lengths, pltpu.HBM)
        out, kv, first = front(size, x, w_query, w_key, w_value, k_cache, v_cache, w_out, lengths)
        return write(*out_product(size, out, kv, first, x, w_out))

    rows_spec = P("replica")
    return jax.shard_map(
        local_step,
        mesh=mesh,
        in_specs=(P("replica", None), P(None, "model"), P(), P(), P("model", None), rows_spec, rows_spec, rows_spec),
        out_specs=(rows_spec, rows_spec, rows_spec),
        check_vma=False,
    )
```
